32 devices in a mesh: grp: 2 (over core), dev: 16 (over z, y, x).
Axes of the slice: x: 2, y: 2, z: 4, core: 2. Of those that a mesh axis runs over, the one named last changes fastest.
Arguments:
- pixel_tiles: float32 [2048, 6, 512], P(('grp', 'dev')), may hold values from -31 to 31
- blend_source: int32 [2048, 2], P(('grp', 'dev')), may hold values from 0 to 15, all different within a row; in each aligned block of 64 rows (0 to 63, 64 to 127, ...) at most 8 rows name the same one
- blend_slot: int32 [2048, 2], P(('grp', 'dev')), may hold values from 0 to 63
- component_count: int32 [2048], P(('grp', 'dev')), may hold values from 12 to 24
- sed_start: bfloat16 [2048, 24, 6], P(('grp', 'dev')), may hold values from 0.049804688 to 0.5
- morph_start: bfloat16 [2048, 2, 24, 512], P(('grp', 'dev')), may hold values from 0.019897461 to 0.5
Outputs:
- whitened: float32 [2048, 6, 512], P(('grp', 'dev'))
- sed_final: bfloat16 [2048, 24, 6], P(('grp', 'dev'))
The draws below stay inside these ranges and needn't reach their ends.
Inputs may be any that keep to these rules, and one draw needn't show every extreme that they name: `blend_source`: each blend names 2 different devices of its region; over the blends of one device no device is named more than 8 times, and some device is named exactly 8 times. `blend_slot`: several blends may name the same tile.
All inputs are finite; a program needn't handle non-finite values.
Results may differ from the reference program's by a relative error of at most 0.0052.
Values may be sent and summed in bfloat16 or wider, within the bound.
A program may use at most 64 MiB of HBM per device.

```python
import math
import jax
import jax.numpy as jnp
import numpy as np
from jax import lax

BANDS = 6
COMPONENTS = 24
PIX = 512
FOOT = 2
ITERS = 2
TILE_DEV = 64
BLEND_DEV = 64
CAPACITY = 8
TILES_G = 1024
BLENDS_G = 1024
TILES_ALL = 2048
BLENDS_ALL = 2048
N_DEV = 16


def draw_pixel_tiles(key, part):
    key_base, key_rough = jax.random.split(jax.random.fold_in(key, 11), 2)
    shape = (TILES_ALL, BANDS, PIX)
    position = (jnp.arange(TILES_ALL, dtype=jnp.int32) % TILES_G).astype(jnp.float32) / TILES_G
    rough = jnp.exp(jax.random.uniform(key_rough, (TILES_ALL, 1, 1), jnp.float32, -0.7, 0.7))
    scale = jnp.power(3.0, position)[:, None, None] * rough
    base = jnp.clip(jax.random.normal(key_base, shape, jnp.float32), -5.0, 5.0)
    return (base * scale).astype(jnp.float32)


def with_ends(drawn, stream_key, low, top_value):
    index_at = [jax.random.randint(jax.random.fold_in(stream_key, axis), (), 0, length) for axis, length in enumerate(drawn.shape)]
    widest = drawn.shape.index(max(drawn.shape))
    next_to = index_at[:widest] + [(index_at[widest] + 1) % drawn.shape[widest]] + index_at[widest + 1:]
    return drawn.at[tuple(index_at)].set(low).at[tuple(next_to)].set(top_value)


def levels(stream_key, extent, pieces, smallest, high):
    def one(axis_at, parts):
        heights = jax.random.uniform(jax.random.fold_in(jax.random.fold_in(stream_key, 6), axis_at), (parts,), jnp.float32, smallest / len(pieces), high / len(pieces))
        return jnp.repeat(jnp.exp(heights), extent[axis_at] // parts).reshape((-1,) + (1,) * (len(extent) - axis_at - 1))

    factor_of = one(*pieces[0])
    for cut in pieces[1:]:
        factor_of = factor_of * one(*cut)
    return factor_of


def shared_out(rng, own, number, rows, amount, top, most, skew):
    sequence = jax.random.permutation(rng, amount)
    packed, ordinary = load_shares(amount, rows * top, most, skew, True), load_shares(amount, rows * top, most, skew, False)
    places = jnp.arange(amount)

    def named(tallies, turn):
        used = int((tallies > 0).sum())
        fixed = max(1, used // 4)
        shifted = fixed + (places - fixed + turn * (used - fixed)) % max(1, amount - fixed)
        return jnp.zeros((amount,), jnp.int32).at[sequence[jnp.where(places < fixed, places, shifted)]].set(jnp.asarray(tallies, jnp.int32))

    tallies = jnp.where(number % 4 == 0, named(packed, number // 4), named(ordinary, number - number // 4 - 1))
    mixed = jax.random.permutation(jax.random.fold_in(own, 3), amount)
    donor, taker = mixed[0:amount // 2 * 2:2], mixed[1:amount // 2 * 2:2]
    slack = jnp.minimum(tallies[donor] - 1, most - tallies[taker]) // 2
    slack = jnp.where((donor == sequence[0]) | (taker == sequence[0]) | (tallies[taker] == 0), 0, jnp.maximum(slack, 0))
    shifted = jax.random.randint(jax.random.fold_in(own, 4), (amount // 2,), 0, 1 << 20) % (slack + 1)
    tallies = tallies.at[donor].add(-shifted).at[taker].add(shifted)
    labels = jnp.searchsorted(jnp.cumsum(tallies), jnp.arange(rows * top), side="right").astype(jnp.int32)
    listing = labels.reshape(top, rows).T
    listing = listing[jax.random.permutation(jax.random.fold_in(own, 1), rows)]
    turn = jax.random.randint(jax.random.fold_in(own, 2), (rows, 1), 0, top)
    return jnp.take_along_axis(listing, (jnp.arange(top)[None, :] + turn) % top, axis=1)


def load_shares(number_of, total, limit, skew, full):
    weights = [(1 << 20) // math.isqrt(grade ** skew) + 1 for grade in range(1, number_of + 1)]
    largest = limit if full else min(limit, max(-(-total // number_of), total * weights[0] // sum(weights)))
    least = 1 if total - largest >= number_of - 1 else 0
    counts, spare = [largest] + [least] * (number_of - 1), total - largest - least * (number_of - 1)
    while spare > 0:
        movable = [i for i in range(1, number_of) if counts[i] < largest] or [i for i in range(1, number_of) if counts[i] < limit]
        mass, left = sum([weights[i] for i in movable]), spare
        for i in movable:
            more = min(limit - counts[i], max(1, left * weights[i] // mass), spare)
            counts[i] = counts[i] + more
            spare = spare - more
    return np.array(counts)


def setup_inputs(seed: int = 0) -> dict:
    streams_of = jax.random.split(jax.random.key(seed), 7)
    pixel_tiles = draw_pixel_tiles(jax.random.fold_in(streams_of[6], 71), 0)
    blend_source_keys = jax.random.split(jax.random.fold_in(streams_of[1], 1), BLENDS_ALL // BLEND_DEV)
    blend_source_turns = jax.random.permutation(jax.random.fold_in(streams_of[1], 3), BLENDS_ALL // BLEND_DEV)
    blend_source = jax.vmap(lambda own, number: shared_out(jax.random.fold_in(streams_of[1], 2), own, number, BLEND_DEV, N_DEV, FOOT, CAPACITY, 2))(blend_source_keys, blend_source_turns).reshape((BLENDS_ALL, FOOT))
    blend_slot = with_ends(jax.random.randint(streams_of[2], (BLENDS_ALL, FOOT), 0, TILE_DEV), jax.random.fold_in(streams_of[2], 1), 0, TILE_DEV - 1).astype(jnp.int32)
    component_count = with_ends(jax.random.randint(streams_of[3], (BLENDS_ALL,), COMPONENTS // 2, COMPONENTS + 1), jax.random.fold_in(streams_of[3], 1), COMPONENTS // 2, COMPONENTS).astype(jnp.int32)
    sed_start = jnp.clip(jnp.exp(math.log(0.5) - 2.306499 * jax.random.uniform(streams_of[4], (BLENDS_ALL, COMPONENTS, BANDS), jnp.float32) ** levels(streams_of[4], (BLENDS_ALL, COMPONENTS, BANDS), ((0, 32),), -0.2, 0.2)), 0.049804688, 0.5).astype(jnp.bfloat16)
    morph_start = jnp.clip(jnp.exp(math.log(0.5) - 3.224016 * jax.random.uniform(streams_of[5], (BLENDS_ALL, FOOT, COMPONENTS, PIX), jnp.float32) ** levels(streams_of[5], (BLENDS_ALL, FOOT, COMPONENTS, PIX), ((0, 32),), -0.2, 0.2)), 0.019897461, 0.5).astype(jnp.bfloat16)
    return dict(pixel_tiles=pixel_tiles, blend_source=blend_source, blend_slot=blend_slot, component_count=component_count, sed_start=sed_start, morph_start=morph_start)


def to_bf16(values):
    return lax.optimization_barrier(values.astype(jnp.bfloat16)).astype(jnp.float32)

def fit_block(blend_data, sed, morph, count):
    active = (jnp.arange(COMPONENTS, dtype=jnp.int32)[None, :] < count[:, None]).astype(jnp.float32)
    sed = sed.astype(jnp.float32) * active[:, :, None]
    morph = morph.astype(jnp.float32) * active[:, None, :, None]
    target = blend_data.astype(jnp.float32)
    for sweep in range(ITERS):
        misfit = to_bf16(jnp.einsum('nkb,nfkp->nfbp', sed, morph) - target)
        gram_matrix = jnp.einsum('nfkp,nfjp->nkj', morph, morph)
        lip_sed = jnp.sqrt(lax.optimization_barrier(jnp.sum(gram_matrix * gram_matrix, axis=(1, 2)))) + 1.0
        gradient = jnp.einsum('nfkp,nfbp->nkb', morph, misfit)
        sed = to_bf16(jnp.maximum(sed - gradient / lip_sed[:, None, None], 0.0) * active[:, :, None])
        misfit = to_bf16(jnp.einsum('nkb,nfkp->nfbp', sed, morph) - target)
        sed_gram = jnp.einsum('nkb,nkc->nbc', sed, sed)
        lip_morph = jnp.sqrt(lax.optimization_barrier(jnp.sum(sed_gram * sed_gram, axis=(1, 2)))) + 1.0
        grad_morph = jnp.einsum('nkb,nfbp->nfkp', sed, misfit)
        morph = to_bf16(jnp.maximum(morph - (grad_morph + 0.1) / lip_morph[:, None, None, None], 0.0) * active[:, None, :, None])
    model_out = jnp.einsum('nkb,nfkp->nfbp', sed, morph).astype(jnp.bfloat16)
    return (sed.astype(jnp.bfloat16), model_out)

def reference(pixel_tiles, blend_source, blend_slot, component_count, sed_start, morph_start):
    group_of = jnp.arange(BLENDS_ALL, dtype=jnp.int32) // BLENDS_G
    tile_index = (group_of[:, None] * TILES_G + blend_source * TILE_DEV + blend_slot).astype(jnp.int32)
    blocks = BLENDS_ALL // BLEND_DEV

    def visit(summed, inputs):
        rows, sed, morph, count = inputs
        blend_data = pixel_tiles[rows].astype(jnp.bfloat16)
        sed_new, model_out = fit_block(blend_data, sed, morph, count)
        summed = summed.at[rows.reshape(-1)].add(model_out.reshape(-1, BANDS, PIX).astype(jnp.float32))
        return (summed, sed_new)
    summed, sed_blocks = lax.scan(visit, jnp.zeros((TILES_ALL, BANDS, PIX), jnp.float32), (tile_index.reshape(blocks, BLEND_DEV, FOOT), sed_start.reshape(blocks, BLEND_DEV, COMPONENTS, BANDS), morph_start.reshape(blocks, BLEND_DEV, FOOT, COMPONENTS, PIX), component_count.reshape(blocks, BLEND_DEV)))
    residual = pixel_tiles - summed
    total_sq = jnp.sum(residual * residual)
    whitened = residual / jnp.sqrt(total_sq / float(TILES_ALL * BANDS * PIX) + 1e-06)
    return (whitened, sed_blocks.reshape(BLENDS_ALL, COMPONENTS, BANDS))
```

```python
import functools
import math

import jax
import jax.numpy as jnp
from jax import lax
from jax.experimental import pallas as pl
from jax.experimental.pallas import tpu as pltpu
from jax.sharding import PartitionSpec as P

INWARD = 1
OUTWARD = 2
F32 = jnp.float32
BF16 = jnp.bfloat16
MESH = pl.DeviceIdType.MESH


def dot(a, b):
    return jnp.dot(a, b, preferred_element_type=F32)


def dot_nt(a, b):
    return lax.dot_general(a, b, (((1,), (1,)), ((), ())), preferred_element_type=F32)


def iota(shape, dimension):
    return lax.broadcasted_iota(jnp.int32, shape, dimension)


def split_row(shape, dimension, width):
    place = iota(shape, dimension)
    out = jnp.zeros(shape, jnp.int32)
    for cut in range(width, shape[dimension], width):
        out = out + (place >= cut).astype(jnp.int32)
    return out, place - out * width


def tgt_depth(width, span):
    return (width + span) // 16 * 16 + 16


def kernel(
    peers, regions, stride, size, tiles, source, slot, count, sed0, morph_hbm, white, sed_out, scale_out,
    morph_in, fit, gram, seds, sed_step, move, mod, pt, ptt, req, wanted, send, arrived, outb, ret, part, parts,
    in_sem, ask_s, ask_r, put_s, put_r, back_s, back_r, sum_s, sum_r,
):
    bands, tile_rows, pixels = tiles.shape
    foot, rows = source.shape
    comps = sed0.shape[1]
    groups = rows // size
    slots = peers * stride
    me = lax.axis_index("dev")
    everyone = peers * regions
    my = lax.axis_index("grp") * peers + me
    load = pltpu.make_async_copy(morph_hbm, morph_in, in_sem)
    load.start()
    barrier = pltpu.get_barrier_semaphore()

    def greet(step, carry):
        other = lax.rem(my + step, everyone)
        pl.semaphore_signal(
            barrier, inc=1, device_id={"grp": lax.div(other, peers), "dev": lax.rem(other, peers)},
            device_id_type=MESH,
        )
        return carry

    lax.fori_loop(1, everyone, greet, 0)

    upper = (iota((rows, rows), 0) <= iota((rows, rows), 1)).astype(F32).astype(BF16)
    base = jnp.zeros((peers, 1), F32)
    want = jnp.zeros((slots, 1), F32)
    for f in range(foot):
        named = source[f : f + 1, :]
        hit = (iota((peers, rows), 0) == named).astype(F32)
        seen = dot(hit.astype(BF16), upper) + base
        rank = jnp.sum(hit * (seen - 1.0), axis=0, keepdims=True)
        base = base + jnp.sum(hit, axis=1, keepdims=True)
        place = named.astype(F32) * float(stride) + rank
        put = (iota((slots, rows), 0).astype(F32) == place).astype(F32)
        pt[f] = put.astype(BF16)
        ptt[f] = jnp.transpose(put).astype(BF16)
        want = want + jnp.sum(put * (slot[f : f + 1, :].astype(F32) + 1.0), axis=1, keepdims=True)
    req[...] = (
        jnp.broadcast_to(want, (slots, 128)).astype(jnp.int32).reshape(peers, stride, 128)
    )
    pl.semaphore_wait(barrier, everyone - 1)

    def exchange(src, dst, send_sem, recv_sem, lanes=None, at=None):
        def part_of(ref, index):
            return ref.at[index] if lanes is None else ref.at[index, :, lanes]

        def sem(ref, step):
            return ref.at[step] if at is None else ref.at[at, step]

        def copy(step, incoming):
            there = lax.rem(me + step, peers)
            here = lax.rem(me - step + peers, peers) if incoming else me
            return pltpu.make_async_remote_copy(
                src_ref=part_of(src, there), dst_ref=part_of(dst, here),
                send_sem=sem(send_sem, step), recv_sem=sem(recv_sem, step),
                device_id={"dev": there}, device_id_type=MESH,
            )

        def start():
            def body(step, carry):
                copy(step, False).start()
                return carry

            lax.fori_loop(1, peers, body, 0)

        def wait_in():
            def body(step, carry):
                copy(step, True).wait_recv()
                return carry

            lax.fori_loop(1, peers, body, 0)

        def wait_out():
            def body(step, carry):
                copy(step, False).wait_send()
                return carry

            lax.fori_loop(1, peers, body, 0)

        return start, wait_in, wait_out

    ask, ask_in, ask_out = exchange(req, wanted, ask_s, ask_r)
    ask()
    wanted[me] = req[me]

    width = size * comps
    span = size * bands
    used = width + span
    depth = tgt_depth(width, span)
    blend_row, comp_row = split_row((width, 1), 0, comps)
    blend_col, comp_col = split_row((1, width), 1, comps)
    band_row, member_row = split_row((span, 1), 0, size)
    same = (blend_row == blend_col).astype(F32)
    same_t = (member_row == blend_col).astype(F32)
    members = (iota((size, width), 0) == blend_col).astype(F32)
    unit = (iota((span, depth), 0) + width == iota((span, depth), 1)).astype(F32)
    lift = (iota((size, depth), 1) == used).astype(F32)
    gather_k = (iota((comps, width), 0) == comp_col).astype(F32).astype(BF16)
    sed_all = jnp.concatenate([sed0[b].astype(F32) for b in range(bands)], axis=1).astype(BF16)
    band_of, blend_of = split_row((1, bands * rows), 1, rows)
    counts = jnp.broadcast_to(count[...], (8, rows)).astype(F32).astype(BF16)

    def chosen(g):
        hit = (band_of == band_row) & (blend_of == g * size + member_row)
        return hit.astype(F32).astype(BF16)

    def every_band(column):
        return jnp.concatenate([column] * bands, axis=0)

    def sed_stepsize(total):
        flat = jnp.sum(total * total, axis=0, keepdims=True)
        return 1.0 / (jnp.sqrt(jnp.sum(members * flat, axis=1, keepdims=True)) + 1.0)

    def wide(column):
        return jnp.broadcast_to(column, (column.shape[0], 128))

    def over_groups(body, pair):
        pair = math.gcd(groups, pair)

        def some(j, carry):
            stores = []
            for k in range(pair):
                stores = stores + body(j * pair + k)
            for ref, index, value in stores:
                ref[index] = value
            return carry

        lax.fori_loop(0, groups // pair, some, 0)

    load.wait()

    def begin(g):
        held = jnp.sum(
            jnp.where(iota((width, rows), 1) == g * size + blend_row, count[...], 0).astype(F32),
            axis=1, keepdims=True,
        )
        active = (comp_row.astype(F32) < held).astype(F32)
        owner = (iota((rows, width), 0) == g * size + blend_col).astype(F32).astype(BF16)
        active_t = (comp_col.astype(F32) < dot(counts, owner)[0:1]).astype(F32)
        first = dot_nt(chosen(g), sed_all)
        stores = [(seds, g, dot(first.astype(BF16), gather_k) * same_t * active_t)]
        tail = (iota((depth - used, pixels), 0) == 0).astype(F32).astype(BF16)
        for f in range(foot):
            whole = morph_in[pl.ds(g * size, size), f].astype(F32).reshape(width, pixels)
            stores.append((fit, (g, f, slice(0, width)), (whole * active).astype(BF16)))
            stores.append((fit, (g, f, slice(used, depth)), tail))
        return stores

    over_groups(begin, 2)
    ask_in()
    picks = (wanted[...].reshape(slots, 128)[:, :tile_rows] - 1 == iota((slots, tile_rows), 1)).astype(F32)
    pick = picks.astype(BF16)
    arrivals = INWARD if bands % INWARD == 0 else 1
    each = bands // arrivals
    fetches = []
    for c in range(arrivals):
        for b in range(c * each, (c + 1) * each):
            block = dot(pick, tiles[b].astype(BF16))
            send[:, :, b * pixels : (b + 1) * pixels] = block.reshape(
                peers, stride, pixels
            ).astype(BF16)
        lanes = slice(c * each * pixels, (c + 1) * each * pixels)
        fetches.append(exchange(send, arrived, put_s, put_r, lanes, c))
        fetches[-1][0]()
    arrived[me] = send[me]

    def morph_of(g, f):
        return fit[g, f, 0:width]

    def first_gram(g):
        total = dot_nt(morph_of(g, 0), morph_of(g, 0))
        for f in range(1, foot):
            total = total + dot_nt(morph_of(g, f), morph_of(g, f))
        total = total * same
        return [(gram, g, total.astype(BF16)), (sed_step, g, wide(sed_stepsize(total)))]

    over_groups(first_gram, 2)

    for c in range(arrivals):
        fetches[c][1]()
        for b in range(c * each, (c + 1) * each):
            block = arrived[:, :, b * pixels : (b + 1) * pixels].astype(F32)
            block = block.reshape(slots, pixels).astype(BF16)
            for f in range(foot):
                at = width + b * size
                fit[:, f, at : at + size, :] = (
                    dot(ptt[f], block).astype(BF16).reshape(groups, size, pixels)
                )

    def first_seds(g):
        cross = dot_nt(fit[g, 0, width:used], morph_of(g, 0))
        for f in range(1, foot):
            cross = cross + dot_nt(fit[g, f, width:used], morph_of(g, f))
        old = seds[g]
        slope = dot(old.astype(BF16), gram[g]) - cross * same_t
        sed = jnp.maximum(old - slope * every_band(sed_step[g, :, 0:1]), 0.0).astype(BF16)
        return [(seds, g, sed.astype(F32))]

    def plan_move(g):
        sed = seds[g]
        held = sed.astype(BF16)
        small = dot_nt(held, held)
        flat = jnp.sum(small * small, axis=1, keepdims=True).reshape(bands, size, 1)
        step = 1.0 / (jnp.sqrt(jnp.sum(flat, axis=0)) + 1.0)
        blank = jnp.zeros((span, depth - width), F32)
        right = (unit - jnp.concatenate([sed, blank], axis=1)) * every_band(step)
        right = jnp.concatenate([right, lift * (-0.1 * step)], axis=0).astype(BF16)
        left = jnp.transpose(jnp.concatenate([sed, members], axis=0)).astype(BF16)
        return [(move, g, dot(left, right).astype(BF16))]

    def moved(g, f, lanes):
        shift = dot(move[g], fit[g, f, :, lanes])
        return jnp.maximum(fit[g, f, 0:width, lanes].astype(F32) + shift, 0.0).astype(BF16)

    def first_morphs(g):
        lanes = slice(0, pixels)
        return [(fit, (g, f, slice(0, width)), moved(g, f, lanes)) for f in range(foot)]

    def second_seds(g):
        total = dot_nt(fit[g, 0, 0:used], morph_of(g, 0))
        for f in range(1, foot):
            total = total + dot_nt(fit[g, f, 0:used], morph_of(g, f))
        cross = total[width:used] * same_t
        total = total[0:width] * same
        old = seds[g]
        slope = dot(old.astype(BF16), total.astype(BF16)) - cross
        sed = jnp.maximum(old - slope * every_band(sed_stepsize(total)), 0.0).astype(BF16)
        return [(seds, g, sed.astype(F32))]

    over_groups(first_seds, 4)
    over_groups(plan_move, 4)
    over_groups(first_morphs, 2)
    over_groups(second_seds, 4)
    over_groups(plan_move, 4)

    window = pixels // OUTWARD
    trips = []
    for chunk in range(OUTWARD):
        taken = slice(chunk * window, (chunk + 1) * window)

        def last_models(g):
            sed = seds[g].astype(BF16)
            stores = []
            for f in range(foot):
                model = dot(sed, moved(g, f, taken)).reshape(bands, size, window)
                member = pl.ds(pl.multiple_of(g * size, size), size)
                stores.append((mod, (f, slice(None), member, slice(None)), model))
            return stores

        over_groups(last_models, 2)
        for b in range(bands):
            block = dot(pt[0], mod[0, b].astype(BF16))
            for f in range(1, foot):
                block = block + dot(pt[f], mod[f, b].astype(BF16))
            at = (chunk * bands + b) * window
            outb[:, :, at : at + window] = block.reshape(peers, stride, window).astype(BF16)
        lanes = slice(chunk * bands * window, (chunk + 1) * bands * window)
        trips.append(exchange(outb, ret, back_s, back_r, lanes, chunk))
        trips[-1][0]()
    ret[me] = outb[me]

    def place(g, placed):
        lean = dot_nt(gather_k, seds[g].astype(BF16))
        return placed + dot(lean.astype(BF16), chosen(g))

    placed = lax.fori_loop(0, groups, place, jnp.zeros((comps, bands * rows), F32))
    for b in range(bands):
        sed_out[b] = placed[:, b * rows : (b + 1) * rows].astype(BF16)
    pick_t = jnp.transpose(picks).astype(BF16)
    squares = jnp.zeros((8, 128), F32)
    for chunk in range(OUTWARD):
        trips[chunk][1]()
        taken = slice(chunk * window, (chunk + 1) * window)
        for b in range(bands):
            at = (chunk * bands + b) * window
            block = ret[:, :, at : at + window].astype(F32).reshape(slots, window).astype(BF16)
            residual = tiles[b, :, taken] - dot(pick_t, block)
            white[b, :, taken] = residual
            square = residual * residual
            for r in range(0, tile_rows, 8):
                for c in range(0, window, 128):
                    squares = squares + square[r : r + 8, c : c + 128]

    own_row = jnp.sum(squares, axis=0, keepdims=True)
    part[...] = own_row

    def share(step, incoming):
        there = lax.rem(my + step, everyone)
        here = lax.rem(my - step + everyone, everyone) if incoming else my
        return pltpu.make_async_remote_copy(
            src_ref=part, dst_ref=parts.at[here], send_sem=sum_s.at[step],
            recv_sem=sum_r.at[step],
            device_id={"grp": lax.div(there, peers), "dev": lax.rem(there, peers)}, device_id_type=MESH,
        )

    def start_share(step, carry):
        share(step, False).start()
        return carry

    def end_share(step, carry):
        share(step, True).wait_recv()
        return carry

    def end_sent(step, carry):
        share(step, False).wait_send()
        return carry

    lax.fori_loop(1, everyone, start_share, 0)
    parts[my] = own_row
    ask_out()
    for trip in fetches + trips:
        trip[2]()
    lax.fori_loop(1, everyone, end_share, 0)
    total = jnp.sum(parts[...], axis=0)
    total = jnp.sum(jnp.sum(total, axis=1, keepdims=True), axis=0, keepdims=True)
    count_all = float(bands * tile_rows * pixels * everyone)
    scale_out[...] = jnp.broadcast_to(1.0 / jnp.sqrt(total / count_all + 1e-06), (8, 128))
    lax.fori_loop(1, everyone, end_sent, 0)


def on_device(pixel_tiles, blend_source, blend_slot, component_count, sed_start, morph_start):
    peers = lax.axis_size("dev")
    regions = lax.axis_size("grp")
    rows, foot = blend_source.shape
    tile_rows, bands, pixels = pixel_tiles.shape
    comps = sed_start.shape[1]
    entries = rows * foot
    capacity = max(2, (entries + peers - 1) // peers)
    stride = (capacity + 7) // 8 * 8
    size = math.gcd(rows, 8)
    groups = rows // size
    slots = peers * stride
    flat = bands * pixels
    depth = tgt_depth(size * comps, size * bands)
    vmem = pl.BlockSpec(memory_space=pltpu.VMEM)
    dma = pltpu.SemaphoreType.DMA
    residual, sed_final, scale = pl.pallas_call(
        functools.partial(kernel, peers, regions, stride, size),
        out_shape=(
            jax.ShapeDtypeStruct((bands, tile_rows, pixels), F32),
            jax.ShapeDtypeStruct((bands, comps, rows), BF16),
            jax.ShapeDtypeStruct((8, 128), F32),
        ),
        in_specs=[vmem] * 5 + [pl.BlockSpec(memory_space=pl.ANY)],
        out_specs=(vmem, vmem, vmem),
        scratch_shapes=[
            pltpu.VMEM(morph_start.shape, BF16),
            pltpu.VMEM((groups, foot, depth, pixels), BF16),
            pltpu.VMEM((groups, size * comps, size * comps), BF16),
            pltpu.VMEM((groups, size * bands, size * comps), F32),
            pltpu.VMEM((groups, size, 128), F32),
            pltpu.VMEM((groups, size * comps, depth), BF16),
            pltpu.VMEM((foot, bands, rows, pixels // OUTWARD), F32),
            pltpu.VMEM((foot, slots, rows), BF16),
            pltpu.VMEM((foot, rows, slots), BF16),
            pltpu.VMEM((peers, stride, 128), jnp.int32),
            pltpu.VMEM((peers, stride, 128), jnp.int32),
            pltpu.VMEM((peers, stride, flat), BF16),
            pltpu.VMEM((peers, stride, flat), BF16),
            pltpu.VMEM((peers, stride, flat), BF16),
            pltpu.VMEM((peers, stride, flat), BF16),
            pltpu.VMEM((1, 128), F32),
            pltpu.VMEM((peers * regions, 1, 128), F32),
            dma,
            dma((peers,)),
            dma((peers,)),
            dma((INWARD, peers)),
            dma((INWARD, peers)),
            dma((OUTWARD, peers)),
            dma((OUTWARD, peers)),
            dma((peers * regions,)),
            dma((peers * regions,)),
        ],
        compiler_params=pltpu.CompilerParams(
            collective_id=0, has_side_effects=True, vmem_limit_bytes=60 * 1024 * 1024
        ),
    )(
        jnp.transpose(pixel_tiles, (1, 0, 2)),
        jnp.transpose(blend_source),
        jnp.transpose(blend_slot),
        component_count.reshape(1, rows),
        jnp.transpose(sed_start, (2, 1, 0)),
        morph_start,
    )
    white = residual * scale[0, 0]
    return jnp.transpose(white, (1, 0, 2)), jnp.transpose(sed_final, (2, 1, 0))


def solution(mesh):
    placed = (
        P(("grp", "dev"), None, None),
        P(("grp", "dev"), None),
        P(("grp", "dev"), None),
        P(("grp", "dev")),
        P(("grp", "dev"), None, None),
        P(("grp", "dev"), None, None, None),
    )
    return jax.shard_map(
        on_device,
        mesh=mesh,
        in_specs=placed,
        out_specs=(P(("grp", "dev"), None, None), P(("grp", "dev"), None, None)),
        check_vma=False,
    )
```

```python
import functools
import math

import jax
import jax.numpy as jnp
from jax import lax
from jax.experimental import pallas as pl
from jax.experimental.pallas import tpu as pltpu
from jax.sharding import PartitionSpec as P

F32 = jnp.float32
BF16 = jnp.bfloat16
MESH = pl.DeviceIdType.MESH


def dot(a, b):
    return jnp.dot(a, b, preferred_element_type=F32)


def dot_nt(a, b):
    return lax.dot_general(a, b, (((1,), (1,)), ((), ())), preferred_element_type=F32)


def iota(shape, dimension):
    return lax.broadcasted_iota(jnp.int32, shape, dimension)


def count_up(shape, dimension):
    return iota(shape, dimension).astype(F32)


def split_row(shape, dimension, width):
    place = iota(shape, dimension)
    out = jnp.zeros(shape, jnp.int32)
    for cut in range(width, shape[dimension], width):
        out = out + (place >= cut).astype(jnp.int32)
    return out, place - out * width


def flag(condition):
    return condition.astype(F32)


def lanes_of(*parts):
    return parts[0] if len(parts) == 1 else jnp.concatenate(parts, axis=1)


def rows_of(*parts):
    return parts[0] if len(parts) == 1 else jnp.concatenate(parts, axis=0)


def tgt_depth(width, span):
    return (width + span) // 16 * 16 + 16


def plan_slots(peers, rows, foot, bands, groups):
    entries = rows * foot
    capacity = max(2, (entries + peers - 1) // peers)
    even = foot == 2 and peers * capacity == entries and capacity % 4 == 0
    halves = 2 if even and groups % 2 == 0 and entries == 128 else 1
    held = capacity // halves
    while held * bands % 8:
        held = held + 1
    return halves, held


def partners(col, row, before, after):
    alike = flag(col == row)
    rank_col = jnp.sum(alike * before, axis=1, keepdims=True)
    rank_row = jnp.sum(alike * after, axis=0, keepdims=True)
    level = flag(jnp.floor(rank_col * 0.5) == jnp.floor(rank_row * 0.5))
    return alike * level * (before + after)


def halve(source_col, source_row, n):
    entries = 2 * n
    before = flag(iota((entries, entries), 1) < iota((entries, entries), 0))
    after = flag(iota((entries, entries), 1) > iota((entries, entries), 0))
    pair = partners(source_col, source_row, before, after)
    step = rows_of(pair[n:], pair[:n]).astype(BF16)
    least = count_up((entries, entries), 0)
    reach = 1
    while reach < n:
        both = dot(step, lanes_of(step, least.astype(BF16)))
        least = jnp.minimum(least, both[:, entries:])
        step = both[:, :entries].astype(BF16)
        reach = reach * 2
    tail = (least[:n] < least[n:])[:, 0:1]
    tail_col = jnp.where(tail, source_col[:n], source_col[n:])
    head_col = jnp.where(tail, source_col[n:], source_col[:n])
    lane = iota((n, 128), 1)
    turned = jnp.transpose(jnp.where(lane == 0, tail_col, jnp.where(lane == 1, head_col, 0.0)))
    before = before[:n, :n]
    after = after[:n, :n]
    tails = partners(tail_col, turned[0:1], before, after).astype(BF16)
    heads = partners(head_col, turned[1:2], before, after).astype(BF16)
    step = dot(tails, heads).astype(BF16)
    least = count_up((n, n), 0)
    reach = 1
    while reach < n // 2:
        least = jnp.minimum(least, dot(step, least.astype(BF16)))
        step = dot(step, step).astype(BF16)
        reach = reach * 2
    return flag(least >= dot(tails, least.astype(BF16)))


def kernel(
    peers, regions, halves, held, size, tiles_hbm, source, slot, count, sed0, morph_hbm, white, sed_out, scale_out,
    tiles, tiles_b, morph_in, fit, gram, seds, sed_step, move, mod, order_v, order_s, req, wanted, send, arrived, outb, ret, part, parts,
    in_sem, ask_s, ask_r, put_s, put_r, back_s, back_r, sum_s, sum_r,
):
    bands, tile_rows, pixels = tiles.shape
    foot, rows = source.shape
    comps = sed0.shape[1]
    groups = rows // size
    per_half = groups // halves
    me = lax.axis_index("dev")
    everyone = peers * regions
    my = lax.axis_index("grp") * peers + me
    load_tiles = pltpu.make_async_copy(tiles_hbm, tiles, in_sem.at[0])
    load_tiles.start()
    load = pltpu.make_async_copy(morph_hbm, morph_in, in_sem.at[1])
    load.start()
    barrier = pltpu.get_barrier_semaphore()

    def greet(step, carry):
        other = lax.rem(my + step, everyone)
        pl.semaphore_signal(
            barrier, inc=1, device_id={"grp": lax.div(other, peers), "dev": lax.rem(other, peers)},
            device_id_type=MESH,
        )
        return carry

    lax.fori_loop(1, everyone, greet, 0)

    entries = foot * rows
    source_row = lanes_of(*[source[f : f + 1, :] for f in range(foot)]).astype(F32)
    slot_row = lanes_of(*[slot[f : f + 1, :] for f in range(foot)]).astype(F32)
    turned = jnp.transpose(rows_of(source_row, slot_row, jnp.zeros((6, entries), F32)))
    source_col = turned[:, 0:1]
    slot_col = turned[:, 1:2]
    before = flag(iota((entries, entries), 1) < iota((entries, entries), 0))
    after = flag(iota((entries, entries), 1) > iota((entries, entries), 0))
    alike = flag(source_col == source_row)
    if halves == 2:
        half = halve(source_col, source_row, rows)
        half_col = half[:, 0:1]
        half_row = jnp.transpose(lanes_of(half, half))[0:1]
        alone = flag(half_col == half_row)
        base = rows // 2
        pos_col = half_col * base + jnp.sum(alone * before[:rows, :rows], axis=1, keepdims=True)
        pos_row = half_row * base + jnp.sum(alone * after[:rows, :rows], axis=0, keepdims=True)
        both_col = rows_of(half_col, half_col)
        both_row = lanes_of(half_row, half_row)
        alike = alike * flag(both_col == both_row)
        rank_col = jnp.sum(alike * before, axis=1, keepdims=True)
        rank_row = jnp.sum(alike * after, axis=0, keepdims=True)
        lane_col = both_col * held + rank_col
    else:
        pos_col = count_up((rows, 1), 0)
        pos_row = count_up((1, rows), 1)
        rank_col = jnp.sum(alike * before, axis=1, keepdims=True)
        rank_row = jnp.sum(alike * after, axis=0, keepdims=True)
        lane_col = rank_col
    named = flag(count_up((peers, entries), 0) == source_row)
    asked = flag(count_up((entries, 128), 1) == lane_col) * (slot_col + 1.0)
    req[...] = dot(named.astype(BF16), asked.astype(BF16)).reshape(peers, 1, 128)
    pl.semaphore_wait(barrier, everyone - 1)

    def exchange(src, dst, send_sem, recv_sem):
        def copy(step, incoming):
            there = lax.rem(me + step, peers)
            here = lax.rem(me - step + peers, peers) if incoming else me
            return pltpu.make_async_remote_copy(
                src_ref=src.at[there], dst_ref=dst.at[here],
                send_sem=send_sem.at[step], recv_sem=recv_sem.at[step],
                device_id={"dev": there}, device_id_type=MESH,
            )

        def start():
            def body(step, carry):
                copy(step, False).start()
                return carry

            lax.fori_loop(1, peers, body, 0)

        def wait_in():
            def body(step, carry):
                copy(step, True).wait_recv()
                return carry

            lax.fori_loop(1, peers, body, 0)

        def wait_out():
            def body(step, carry):
                copy(step, False).wait_send()
                return carry

            lax.fori_loop(1, peers, body, 0)

        return start, wait_in, wait_out

    ask, ask_in, ask_out = exchange(req, wanted, ask_s, ask_r)
    ask()
    wanted[me] = req[me]

    order = jnp.sum(flag(count_up((rows, 128), 1) == pos_col) * count_up((rows, 128), 0), axis=0, keepdims=True)
    order = jnp.minimum(order, float(rows - 1))
    order_v[...] = jnp.broadcast_to(order, (8, 128)).astype(jnp.int32)
    to_scalars = pltpu.make_async_copy(order_v, order_s, in_sem.at[2])
    to_scalars.start()

    width = size * comps
    span = size * bands
    used = width + span
    depth = tgt_depth(width, span)
    blend_row, comp_row = split_row((width, 1), 0, comps)
    blend_col, comp_col = split_row((1, width), 1, comps)
    band_row, member_row = split_row((span, 1), 0, size)
    same = flag(blend_row == blend_col)
    same_t = flag(member_row == blend_col)
    members = flag(iota((size, width), 0) == blend_col)
    unit = flag(iota((span, depth), 0) + width == iota((span, depth), 1))
    lift = flag(iota((size, depth), 1) == used)
    eye = flag(iota((width, width), 0) == iota((width, width), 1)).astype(BF16)
    gather_k = flag(iota((comps, width), 0) == comp_col).astype(BF16)
    sed_all = jnp.concatenate([sed0[b].astype(F32) for b in range(bands)], axis=1).astype(BF16)
    band_of, _ = split_row((1, bands * rows), 1, rows)
    pos_of = lanes_of(*[pos_row] * bands)
    counts = jnp.broadcast_to(count[...], (8, rows)).astype(F32).astype(BF16)

    def chosen(g):
        hit = (band_of == band_row) & (pos_of == (g * size + member_row).astype(F32))
        return flag(hit).astype(BF16)

    def every_band(column):
        return jnp.concatenate([column] * bands, axis=0)

    def sed_stepsize(total):
        flat = jnp.sum(total * total, axis=0, keepdims=True)
        return 1.0 / (jnp.sqrt(jnp.sum(members * flat, axis=1, keepdims=True)) + 1.0)

    def wide(column):
        return jnp.broadcast_to(column, (column.shape[0], 128))

    def over_groups(body, first, number, pair):
        pair = math.gcd(number, pair)

        def some(j, carry):
            stores = []
            for k in range(pair):
                stores = stores + body(first + j * pair + k)
            for ref, index, value in stores:
                ref[index] = value
            return carry

        lax.fori_loop(0, number // pair, some, 0)

    to_scalars.wait()
    load.wait()

    def begin(g):
        mine = pos_row == (g * size + blend_row).astype(F32)
        kept = jnp.sum(jnp.where(mine, count[...].astype(F32), 0.0), axis=1, keepdims=True)
        active = flag(comp_row.astype(F32) < kept)
        owner = flag(pos_col == (g * size + blend_col).astype(F32)).astype(BF16)
        active_t = flag(comp_col.astype(F32) < dot(counts, owner)[0:1])
        first = dot_nt(chosen(g), sed_all)
        stores = [(seds, g, dot(first.astype(BF16), gather_k) * same_t * active_t)]
        tail = flag(iota((depth - used, pixels), 0) == 0).astype(BF16)
        places = [jnp.clip(order_s[0, g * size + m], 0, rows - 1) for m in range(size)]
        for f in range(foot):
            whole = rows_of(*[morph_in[place, f].astype(F32) for place in places])
            stores.append((fit, (g, f, slice(0, width)), (whole * active).astype(BF16)))
            stores.append((fit, (g, f, slice(used, depth)), tail))
        return stores

    over_groups(begin, 0, groups, 2)
    load_tiles.wait()
    tiles_b[...] = tiles[...].reshape(bands * tile_rows, pixels).astype(BF16)

    team = math.gcd(peers, 16)
    each = bands * held
    crowd = team * each
    stock = bands * tile_rows
    teams = [slice(k, k + team) for k in range(0, peers, team)]
    _, seat_row = split_row((crowd, 1), 0, each)
    seat_band_row, seat_rank_row = split_row((crowd, 1), 0, held)
    peer_col, seat_col = split_row((1, crowd), 1, each)
    seat_band_row = seat_band_row - split_row((crowd, 1), 0, each)[0] * bands
    seat_band_col, seat_rank_col = split_row((1, crowd), 1, held)
    seat_band_col = seat_band_col - peer_col * bands

    def pick_of(h, who):
        lines = jnp.broadcast_to(wanted[who], (team, each, 128)).reshape(crowd, 128)
        seat = flag(iota((crowd, 128), 1) == h * held + seat_rank_row)
        tile = jnp.sum(lines * seat, axis=1, keepdims=True)
        at = jnp.where(tile > 0.0, tile - 1.0 + (seat_band_row * tile_rows).astype(F32), -1.0)
        return flag(count_up((crowd, stock), 1) == at).astype(BF16)

    def pick_t_of(h, who):
        lines = wanted[who].reshape(team, 128).astype(BF16)
        seat = flag(iota((128, crowd), 0) == h * held + seat_rank_col).astype(BF16)
        tile = dot(lines, seat) * flag(iota((team, crowd), 0) == peer_col)
        tile = jnp.sum(tile, axis=0, keepdims=True)
        at = jnp.where(tile > 0.0, tile - 1.0 + (seat_band_col * tile_rows).astype(F32), -1.0)
        return flag(count_up((stock, crowd), 0) == at).astype(BF16)

    ask_in()
    fetches = []
    for h in range(halves):
        for who in teams:
            block = dot(pick_of(h, who), tiles_b[...])
            send[h, who] = block.reshape(team, each, pixels).astype(BF16)
        fetches.append(exchange(send.at[h], arrived.at[h], put_s.at[h], put_r.at[h]))
        fetches[h][0]()
        arrived[h, me] = send[h, me]

    def morph_of(g, f):
        return fit[g, f, 0:width]

    def first_gram(g):
        total = dot_nt(morph_of(g, 0), morph_of(g, 0))
        for f in range(1, foot):
            total = total + dot_nt(morph_of(g, f), morph_of(g, f))
        total = total * same
        return [(gram, g, total.astype(BF16)), (sed_step, g, wide(sed_stepsize(total)))]

    over_groups(first_gram, 0, groups, 4)

    crew = per_half * foot * span
    crew_row, crew_band_row = split_row((crew, 1), 0, span)
    crew_band_row, crew_member_row = split_row((crew, 1), 0, size)
    crew_band_row = crew_band_row - crew_row * bands
    crew_col, _ = split_row((1, crew), 1, span)
    crew_band_col, crew_member_col = split_row((1, crew), 1, size)
    crew_band_col = crew_band_col - crew_col * bands
    group_row = split_row((crew, 1), 0, foot * span)[0]
    group_col = split_row((1, crew), 1, foot * span)[0]
    foot_row = crew_row - group_row * foot
    foot_col = crew_col - group_col * foot
    entry_row = lanes_of(*[pos_row + f * rows for f in range(foot)])
    entry_col = rows_of(*[pos_col + f * rows for f in range(foot)])
    facts = lanes_of(
        jnp.broadcast_to(source_col, (entries, 128)), jnp.broadcast_to(rank_col, (entries, 128))
    ).astype(BF16)
    facts_t = rows_of(source_row, rank_row, jnp.zeros((6, entries), F32)).astype(BF16)

    def give_of(h, first):
        here = ((h * per_half + group_row) * size + crew_member_row + foot_row * rows).astype(F32)
        found = dot(flag(here == entry_row).astype(BF16), facts)
        at = (found[:, 0:1] - first) * each + found[:, 128:129] + (crew_band_row * held).astype(F32)
        return flag(count_up((crew, crowd), 1) == at).astype(BF16)

    def give_t_of(h, first):
        here = ((h * per_half + group_col) * size + crew_member_col + foot_col * rows).astype(F32)
        found = dot(facts_t, flag(entry_col == here).astype(BF16))
        at = (found[0:1] - first) * each + found[1:2] + (crew_band_col * held).astype(F32)
        return flag(count_up((crowd, crew), 0) == at).astype(BF16)

    def first_seds(g):
        cross = dot_nt(fit[g, 0, width:used], morph_of(g, 0))
        for f in range(1, foot):
            cross = cross + dot_nt(fit[g, f, width:used], morph_of(g, f))
        old = seds[g]
        slope = dot(old.astype(BF16), gram[g]) - cross * same_t
        sed = jnp.maximum(old - slope * every_band(sed_step[g, :, 0:1]), 0.0).astype(BF16)
        return [(seds, g, sed.astype(F32))]

    def plan_move(g):
        sed = seds[g]
        bold = sed.astype(BF16)
        small = dot_nt(bold, bold)
        flat = jnp.sum(small * small, axis=1, keepdims=True).reshape(bands, size, 1)
        step = 1.0 / (jnp.sqrt(jnp.sum(flat, axis=0)) + 1.0)
        blank = jnp.zeros((span, depth - width), F32)
        right = (unit - jnp.concatenate([sed, blank], axis=1)) * every_band(step)
        right = jnp.concatenate([right, lift * (-0.1 * step)], axis=0).astype(BF16)
        left = dot_nt(eye, jnp.concatenate([sed, members], axis=0).astype(BF16)).astype(BF16)
        return [(move, g, dot(left, right).astype(BF16))]

    def moved(g, f):
        shift = dot(move[g], fit[g, f])
        return jnp.maximum(fit[g, f, 0:width].astype(F32) + shift, 0.0).astype(BF16)

    def first_morphs(g):
        return [(fit, (g, f, slice(0, width)), moved(g, f)) for f in range(foot)]

    def second_seds(g):
        total = dot_nt(fit[g, 0, 0:used], morph_of(g, 0))
        for f in range(1, foot):
            total = total + dot_nt(fit[g, f, 0:used], morph_of(g, f))
        cross = total[width:used] * same_t
        total = total[0:width] * same
        old = seds[g]
        slope = dot(old.astype(BF16), total.astype(BF16)) - cross
        sed = jnp.maximum(old - slope * every_band(sed_stepsize(total)), 0.0).astype(BF16)
        return [(seds, g, sed.astype(F32))]

    def last_models(g):
        sed = seds[g].astype(BF16)
        return [(mod, (g, f), dot(sed, moved(g, f)).astype(BF16)) for f in range(foot)]

    trips = []
    for h in range(halves):
        first = h * per_half
        fetches[h][1]()
        block = jnp.zeros((crew, pixels), F32)
        for k, who in enumerate(teams):
            come = arrived[h, who].astype(F32).reshape(crowd, pixels).astype(BF16)
            block = block + dot(give_of(h, k * team), come)
        block = block.astype(BF16).reshape(per_half, foot, span, pixels)
        fit[first : first + per_half, :, width:used] = block
        over_groups(first_seds, first, per_half, 4)
        over_groups(plan_move, first, per_half, 4)
        over_groups(first_morphs, first, per_half, 4)
        over_groups(second_seds, first, per_half, 4)
        over_groups(plan_move, first, per_half, 4)
        over_groups(last_models, first, per_half, 4)
        models = mod[first : first + per_half].reshape(crew, pixels)
        for k, who in enumerate(teams):
            block = dot(give_t_of(h, k * team), models)
            outb[h, who] = block.reshape(team, each, pixels).astype(BF16)
        trips.append(exchange(outb.at[h], ret.at[h], back_s.at[h], back_r.at[h]))
        trips[h][0]()
        ret[h, me] = outb[h, me]

    def put_back(g, placed):
        lean = dot_nt(gather_k, seds[g].astype(BF16))
        return placed + dot(lean.astype(BF16), chosen(g))

    placed = lax.fori_loop(0, groups, put_back, jnp.zeros((comps, bands * rows), F32))
    for b in range(bands):
        sed_out[b] = placed[:, b * rows : (b + 1) * rows].astype(BF16)

    for h in range(halves):
        trips[h][1]()
        total = jnp.zeros((stock, pixels), F32)
        for who in teams:
            come = ret[h, who].astype(F32).reshape(crowd, pixels).astype(BF16)
            total = total + dot(pick_t_of(h, who), come)
        left = tiles if h == 0 else white
        white[...] = left[...] - total.reshape(bands, tile_rows, pixels)

    squares = jnp.zeros((8, 128), F32)
    for b in range(bands):
        square = white[b] * white[b]
        for r in range(0, tile_rows, 8):
            for c in range(0, pixels, 128):
                squares = squares + square[r : r + 8, c : c + 128]

    own_row = jnp.sum(squares, axis=0, keepdims=True)
    part[...] = own_row

    def share(step, incoming):
        there = lax.rem(my + step, everyone)
        here = lax.rem(my - step + everyone, everyone) if incoming else my
        return pltpu.make_async_remote_copy(
            src_ref=part, dst_ref=parts.at[here], send_sem=sum_s.at[step],
            recv_sem=sum_r.at[step],
            device_id={"grp": lax.div(there, peers), "dev": lax.rem(there, peers)}, device_id_type=MESH,
        )

    def start_share(step, carry):
        share(step, False).start()
        return carry

    def end_share(step, carry):
        share(step, True).wait_recv()
        return carry

    def end_sent(step, carry):
        share(step, False).wait_send()
        return carry

    lax.fori_loop(1, everyone, start_share, 0)
    parts[my] = own_row
    ask_out()
    for trip in fetches + trips:
        trip[2]()
    lax.fori_loop(1, everyone, end_share, 0)
    total = jnp.sum(parts[...], axis=0)
    total = jnp.sum(jnp.sum(total, axis=1, keepdims=True), axis=0, keepdims=True)
    count_all = float(bands * tile_rows * pixels * everyone)
    scale_out[...] = jnp.broadcast_to(1.0 / jnp.sqrt(total / count_all + 1e-06), (8, 128))
    lax.fori_loop(1, everyone, end_sent, 0)


def on_device(pixel_tiles, blend_source, blend_slot, component_count, sed_start, morph_start):
    peers = lax.axis_size("dev")
    regions = lax.axis_size("grp")
    rows, foot = blend_source.shape
    tile_rows, bands, pixels = pixel_tiles.shape
    comps = sed_start.shape[1]
    size = math.gcd(rows, 8)
    groups = rows // size
    halves, held = plan_slots(peers, rows, foot, bands, groups)
    width = size * comps
    span = size * bands
    depth = tgt_depth(width, span)
    vmem = pl.BlockSpec(memory_space=pltpu.VMEM)
    hbm = pl.BlockSpec(memory_space=pl.ANY)
    dma = pltpu.SemaphoreType.DMA
    parcel = pltpu.VMEM((halves, peers, bands * held, pixels), BF16)
    residual, sed_final, scale = pl.pallas_call(
        functools.partial(kernel, peers, regions, halves, held, size),
        out_shape=(
            jax.ShapeDtypeStruct((bands, tile_rows, pixels), F32),
            jax.ShapeDtypeStruct((bands, comps, rows), BF16),
            jax.ShapeDtypeStruct((8, 128), F32),
        ),
        in_specs=[hbm] + [vmem] * 4 + [hbm],
        out_specs=(vmem, vmem, vmem),
        scratch_shapes=[
            pltpu.VMEM((bands, tile_rows, pixels), F32),
            pltpu.VMEM((bands * tile_rows, pixels), BF16),
            pltpu.VMEM(morph_start.shape, BF16),
            pltpu.VMEM((groups, foot, depth, pixels), BF16),
            pltpu.VMEM((groups, width, width), BF16),
            pltpu.VMEM((groups, span, width), F32),
            pltpu.VMEM((groups, size, 128), F32),
            pltpu.VMEM((groups, width, depth), BF16),
            pltpu.VMEM((groups, foot, span, pixels), BF16),
            pltpu.VMEM((8, 128), jnp.int32),
            pltpu.SMEM((8, 128), jnp.int32),
            pltpu.VMEM((peers, 1, 128), F32),
            pltpu.VMEM((peers, 1, 128), F32),
            parcel,
            parcel,
            parcel,
            parcel,
            pltpu.VMEM((1, 128), F32),
            pltpu.VMEM((peers * regions, 1, 128), F32),
            dma((3,)),
            dma((peers,)),
            dma((peers,)),
            dma((halves, peers)),
            dma((halves, peers)),
            dma((halves, peers)),
            dma((halves, peers)),
            dma((peers * regions,)),
            dma((peers * regions,)),
        ],
        compiler_params=pltpu.CompilerParams(
            collective_id=0, has_side_effects=True, vmem_limit_bytes=60 * 1024 * 1024
        ),
    )(
        jnp.transpose(pixel_tiles, (1, 0, 2)),
        jnp.transpose(blend_source),
        jnp.transpose(blend_slot),
        component_count.reshape(1, rows),
        jnp.transpose(sed_start, (2, 1, 0)),
        morph_start,
    )
    white = residual * scale[0, 0]
    return jnp.transpose(white, (1, 0, 2)), jnp.transpose(sed_final, (2, 1, 0))


def solution(mesh):
    placed = (
        P(("grp", "dev"), None, None),
        P(("grp", "dev"), None),
        P(("grp", "dev"), None),
        P(("grp", "dev")),
        P(("grp", "dev"), None, None),
        P(("grp", "dev"), None, None, None),
    )
    return jax.shard_map(
        on_device,
        mesh=mesh,
        in_specs=placed,
        out_specs=(P(("grp", "dev"), None, None), P(("grp", "dev"), None, None)),
        check_vma=False,
    )
```

```python
import functools
import math

import jax
import jax.numpy as jnp
from jax import lax
from jax.experimental import pallas as pl
from jax.experimental.pallas import tpu as pltpu
from jax.sharding import PartitionSpec as P

F32 = jnp.float32
BF16 = jnp.bfloat16
MESH = pl.DeviceIdType.MESH


def dot(a, b):
    return jnp.dot(a, b, preferred_element_type=F32)


def dot_nt(a, b):
    return lax.dot_general(a, b, (((1,), (1,)), ((), ())), preferred_element_type=F32)


def iota(shape, dimension):
    return lax.broadcasted_iota(jnp.int32, shape, dimension)


def count_up(shape, dimension):
    return iota(shape, dimension).astype(F32)


def split_row(shape, dimension, width):
    place = iota(shape, dimension)
    out = jnp.zeros(shape, jnp.int32)
    for cut in range(width, shape[dimension], width):
        out = out + (place >= cut).astype(jnp.int32)
    return out, place - out * width


def flag(condition):
    return condition.astype(F32)


def lanes_of(*parts):
    return parts[0] if len(parts) == 1 else jnp.concatenate(parts, axis=1)


def rows_of(*parts):
    return parts[0] if len(parts) == 1 else jnp.concatenate(parts, axis=0)


def tgt_depth(width, span):
    return (width + span) // 16 * 16 + 16


def plan_slots(peers, rows, foot, bands, groups):
    entries = rows * foot
    capacity = max(2, (entries + peers - 1) // peers)
    even = foot == 2 and peers * capacity == entries and capacity % 4 == 0
    halves = 2 if even and groups % 2 == 0 and entries == 128 else 1
    held = capacity // halves
    while held * bands % 8:
        held = held + 1
    return halves, held


def partners(col, row, before, after):
    alike = flag(col == row)
    rank_col = jnp.sum(alike * before, axis=1, keepdims=True)
    rank_row = jnp.sum(alike * after, axis=0, keepdims=True)
    level = flag(jnp.floor(rank_col * 0.5) == jnp.floor(rank_row * 0.5))
    return alike * level * (before + after)


def halve(source_col, source_row, n):
    entries = 2 * n
    before = flag(iota((entries, entries), 1) < iota((entries, entries), 0))
    after = flag(iota((entries, entries), 1) > iota((entries, entries), 0))
    pair = partners(source_col, source_row, before, after)
    step = rows_of(pair[n:], pair[:n]).astype(BF16)
    least = count_up((entries, entries), 0)
    reach = 1
    while reach < n:
        both = dot(step, lanes_of(step, least.astype(BF16)))
        least = jnp.minimum(least, both[:, entries:])
        step = both[:, :entries].astype(BF16)
        reach = reach * 2
    tail = (least[:n] < least[n:])[:, 0:1]
    tail_col = jnp.where(tail, source_col[:n], source_col[n:])
    head_col = jnp.where(tail, source_col[n:], source_col[:n])
    lane = iota((n, 128), 1)
    turned = jnp.transpose(jnp.where(lane == 0, tail_col, jnp.where(lane == 1, head_col, 0.0)))
    before = before[:n, :n]
    after = after[:n, :n]
    tails = partners(tail_col, turned[0:1], before, after).astype(BF16)
    heads = partners(head_col, turned[1:2], before, after).astype(BF16)
    step = dot(tails, heads).astype(BF16)
    least = count_up((n, n), 0)
    reach = 1
    while reach < n // 2:
        least = jnp.minimum(least, dot(step, least.astype(BF16)))
        step = dot(step, step).astype(BF16)
        reach = reach * 2
    return flag(least >= dot(tails, least.astype(BF16)))


def kernel(
    peers, regions, halves, held, size,
    tiles_hbm, source_hbm, slot_hbm, count_hbm, sed_hbm, morph_hbm, white_out, sed_out, scale_out, source, slot, count, sed0,
    white, sed_made, tiles, tiles_b, morph_in, fit, gram, seds, sed_step, move, mod, give, give_t, pick_t, order_v, order_s, req, wanted, send, arrived, outb, ret, part, parts,
    in_sem, ask_s, ask_r, put_s, put_r, back_s, back_r, sum_s, sum_r,
):
    bands, tile_rows, pixels = tiles.shape
    foot, rows = source.shape
    comps = sed0.shape[1]
    groups = rows // size
    per_half = groups // halves
    me = lax.axis_index("dev")
    everyone = peers * regions
    my = lax.axis_index("grp") * peers + me
    small = [
        pltpu.make_async_copy(given, kept, in_sem.at[3 + i])
        for i, (given, kept) in enumerate(
            ((source_hbm, source), (slot_hbm, slot), (count_hbm, count), (sed_hbm, sed0))
        )
    ]
    for copy in small:
        copy.start()
    load_tiles = pltpu.make_async_copy(tiles_hbm, tiles, in_sem.at[0])
    load_tiles.start()
    load = pltpu.make_async_copy(morph_hbm, morph_in, in_sem.at[1])
    load.start()
    barrier = pltpu.get_barrier_semaphore()

    def greet(step, carry):
        other = lax.rem(my + step, everyone)
        pl.semaphore_signal(
            barrier, inc=1, device_id={"grp": lax.div(other, peers), "dev": lax.rem(other, peers)},
            device_id_type=MESH,
        )
        return carry

    lax.fori_loop(1, everyone, greet, 0)

    small[0].wait()
    small[1].wait()
    entries = foot * rows
    source_row = lanes_of(*[source[f : f + 1, :] for f in range(foot)]).astype(F32)
    slot_row = lanes_of(*[slot[f : f + 1, :] for f in range(foot)]).astype(F32)
    turned = jnp.transpose(rows_of(source_row, slot_row, jnp.zeros((6, entries), F32)))
    source_col = turned[:, 0:1]
    slot_col = turned[:, 1:2]
    before = flag(iota((entries, entries), 1) < iota((entries, entries), 0))
    after = flag(iota((entries, entries), 1) > iota((entries, entries), 0))
    alike = flag(source_col == source_row)
    if halves == 2:
        half = halve(source_col, source_row, rows)
        half_col = half[:, 0:1]
        half_row = jnp.transpose(lanes_of(half, half))[0:1]
        alone = flag(half_col == half_row)
        base = rows // 2
        pos_col = half_col * base + jnp.sum(alone * before[:rows, :rows], axis=1, keepdims=True)
        pos_row = half_row * base + jnp.sum(alone * after[:rows, :rows], axis=0, keepdims=True)
        both_col = rows_of(half_col, half_col)
        both_row = lanes_of(half_row, half_row)
        alike = alike * flag(both_col == both_row)
        rank_col = jnp.sum(alike * before, axis=1, keepdims=True)
        rank_row = jnp.sum(alike * after, axis=0, keepdims=True)
        lane_col = both_col * held + rank_col
    else:
        pos_col = count_up((rows, 1), 0)
        pos_row = count_up((1, rows), 1)
        rank_col = jnp.sum(alike * before, axis=1, keepdims=True)
        rank_row = jnp.sum(alike * after, axis=0, keepdims=True)
        lane_col = rank_col
    named = flag(count_up((peers, entries), 0) == source_row)
    asked = flag(count_up((entries, 128), 1) == lane_col) * (slot_col + 1.0)
    req[...] = dot(named.astype(BF16), asked.astype(BF16)).reshape(peers, 1, 128)
    pl.semaphore_wait(barrier, everyone - 1)

    def exchange(src, dst, send_sem, recv_sem):
        def copy(step, incoming):
            there = lax.rem(me + step, peers)
            here = lax.rem(me - step + peers, peers) if incoming else me
            return pltpu.make_async_remote_copy(
                src_ref=src.at[there], dst_ref=dst.at[here],
                send_sem=send_sem.at[step], recv_sem=recv_sem.at[step],
                device_id={"dev": there}, device_id_type=MESH,
            )

        def start():
            def body(step, carry):
                copy(step, False).start()
                return carry

            lax.fori_loop(1, peers, body, 0)

        def wait_in():
            def body(step, carry):
                copy(step, True).wait_recv()
                return carry

            lax.fori_loop(1, peers, body, 0)

        def wait_out():
            def body(step, carry):
                copy(step, False).wait_send()
                return carry

            lax.fori_loop(1, peers, body, 0)

        return start, wait_in, wait_out

    ask, ask_in, ask_out = exchange(req, wanted, ask_s, ask_r)
    ask()
    wanted[me] = req[me]

    order = jnp.sum(flag(count_up((rows, 128), 1) == pos_col) * count_up((rows, 128), 0), axis=0, keepdims=True)
    order = jnp.minimum(order, float(rows - 1))
    order_v[...] = jnp.broadcast_to(order, (8, 128)).astype(jnp.int32)
    to_scalars = pltpu.make_async_copy(order_v, order_s, in_sem.at[2])
    to_scalars.start()

    small[2].wait()
    small[3].wait()
    width = size * comps
    span = size * bands
    used = width + span
    depth = tgt_depth(width, span)
    blend_row, comp_row = split_row((width, 1), 0, comps)
    blend_col, comp_col = split_row((1, width), 1, comps)
    band_row, member_row = split_row((span, 1), 0, size)
    same = flag(blend_row == blend_col)
    same_t = flag(member_row == blend_col)
    members = flag(iota((size, width), 0) == blend_col)
    unit = flag(iota((span, depth), 0) + width == iota((span, depth), 1))
    lift = flag(iota((size, depth), 1) == used)
    eye = flag(iota((width, width), 0) == iota((width, width), 1)).astype(BF16)
    gather_k = flag(iota((comps, width), 0) == comp_col).astype(BF16)
    sed_all = jnp.concatenate([sed0[b].astype(F32) for b in range(bands)], axis=1).astype(BF16)
    band_of, _ = split_row((1, bands * rows), 1, rows)
    pos_of = lanes_of(*[pos_row] * bands)
    counts = jnp.broadcast_to(count[...], (8, rows)).astype(F32).astype(BF16)

    def chosen(g):
        hit = (band_of == band_row) & (pos_of == (g * size + member_row).astype(F32))
        return flag(hit).astype(BF16)

    def every_band(column):
        return jnp.concatenate([column] * bands, axis=0)

    def sed_stepsize(total):
        flat = jnp.sum(total * total, axis=0, keepdims=True)
        return 1.0 / (jnp.sqrt(jnp.sum(members * flat, axis=1, keepdims=True)) + 1.0)

    def wide(column):
        return jnp.broadcast_to(column, (column.shape[0], 128))

    def over_groups(body, first, number, pair):
        pair = math.gcd(number, pair)

        def some(j, carry):
            stores = []
            for k in range(pair):
                stores = stores + body(first + j * pair + k)
            for ref, index, value in stores:
                ref[index] = value
            return carry

        lax.fori_loop(0, number // pair, some, 0)

    to_scalars.wait()
    load.wait()

    def begin(g):
        mine = pos_row == (g * size + blend_row).astype(F32)
        kept = jnp.sum(jnp.where(mine, count[...].astype(F32), 0.0), axis=1, keepdims=True)
        active = flag(comp_row.astype(F32) < kept)
        owner = flag(pos_col == (g * size + blend_col).astype(F32)).astype(BF16)
        active_t = flag(comp_col.astype(F32) < dot(counts, owner)[0:1])
        first = dot_nt(chosen(g), sed_all)
        stores = [(seds, g, dot(first.astype(BF16), gather_k) * same_t * active_t)]
        tail = flag(iota((depth - used, pixels), 0) == 0).astype(BF16)
        places = [jnp.clip(order_s[0, g * size + m], 0, rows - 1) for m in range(size)]
        for f in range(foot):
            whole = rows_of(*[morph_in[place, f].astype(F32) for place in places])
            stores.append((fit, (g, f, slice(0, width)), (whole * active).astype(BF16)))
            stores.append((fit, (g, f, slice(used, depth)), tail))
        return stores

    over_groups(begin, 0, groups, 2)
    load_tiles.wait()
    tiles_b[...] = tiles[...].reshape(bands * tile_rows, pixels).astype(BF16)

    team = math.gcd(peers, 16)
    each = bands * held
    crowd = team * each
    stock = bands * tile_rows
    teams = [slice(k, k + team) for k in range(0, peers, team)]
    _, seat_row = split_row((crowd, 1), 0, each)
    seat_band_row, seat_rank_row = split_row((crowd, 1), 0, held)
    peer_col, seat_col = split_row((1, crowd), 1, each)
    seat_band_row = seat_band_row - split_row((crowd, 1), 0, each)[0] * bands
    seat_band_col, seat_rank_col = split_row((1, crowd), 1, held)
    seat_band_col = seat_band_col - peer_col * bands

    def pick_of(h, who):
        lines = jnp.broadcast_to(wanted[who], (team, each, 128)).reshape(crowd, 128)
        seat = flag(iota((crowd, 128), 1) == h * held + seat_rank_row)
        tile = jnp.sum(lines * seat, axis=1, keepdims=True)
        at = jnp.where(tile > 0.0, tile - 1.0 + (seat_band_row * tile_rows).astype(F32), -1.0)
        return flag(count_up((crowd, stock), 1) == at).astype(BF16)

    def pick_t_of(h, who):
        lines = wanted[who].reshape(team, 128).astype(BF16)
        seat = flag(iota((128, crowd), 0) == h * held + seat_rank_col).astype(BF16)
        tile = dot(lines, seat) * flag(iota((team, crowd), 0) == peer_col)
        tile = jnp.sum(tile, axis=0, keepdims=True)
        at = jnp.where(tile > 0.0, tile - 1.0 + (seat_band_col * tile_rows).astype(F32), -1.0)
        return flag(count_up((stock, crowd), 0) == at).astype(BF16)

    ask_in()
    fetches = []
    for h in range(halves):
        for who in teams:
            block = dot(pick_of(h, who), tiles_b[...])
            send[h, who] = block.reshape(team, each, pixels).astype(BF16)
        fetches.append(exchange(send.at[h], arrived.at[h], put_s.at[h], put_r.at[h]))
        fetches[h][0]()
        arrived[h, me] = send[h, me]

    def morph_of(g, f):
        return fit[g, f, 0:width]

    def first_gram(g):
        total = dot_nt(morph_of(g, 0), morph_of(g, 0))
        for f in range(1, foot):
            total = total + dot_nt(morph_of(g, f), morph_of(g, f))
        total = total * same
        return [(gram, g, total.astype(BF16)), (sed_step, g, wide(sed_stepsize(total)))]

    over_groups(first_gram, 0, groups, 4)

    crew = per_half * foot * span
    crew_row, crew_band_row = split_row((crew, 1), 0, span)
    crew_band_row, crew_member_row = split_row((crew, 1), 0, size)
    crew_band_row = crew_band_row - crew_row * bands
    crew_col, _ = split_row((1, crew), 1, span)
    crew_band_col, crew_member_col = split_row((1, crew), 1, size)
    crew_band_col = crew_band_col - crew_col * bands
    group_row = split_row((crew, 1), 0, foot * span)[0]
    group_col = split_row((1, crew), 1, foot * span)[0]
    foot_row = crew_row - group_row * foot
    foot_col = crew_col - group_col * foot
    entry_row = lanes_of(*[pos_row + f * rows for f in range(foot)])
    entry_col = rows_of(*[pos_col + f * rows for f in range(foot)])
    facts = lanes_of(
        jnp.broadcast_to(source_col, (entries, 128)), jnp.broadcast_to(rank_col, (entries, 128))
    ).astype(BF16)
    facts_t = rows_of(source_row, rank_row, jnp.zeros((6, entries), F32)).astype(BF16)

    def give_of(h, first):
        here = ((h * per_half + group_row) * size + crew_member_row + foot_row * rows).astype(F32)
        found = dot(flag(here == entry_row).astype(BF16), facts)
        at = (found[:, 0:1] - first) * each + found[:, 128:129] + (crew_band_row * held).astype(F32)
        return flag(count_up((crew, crowd), 1) == at).astype(BF16)

    def give_t_of(h, first):
        here = ((h * per_half + group_col) * size + crew_member_col + foot_col * rows).astype(F32)
        found = dot(facts_t, flag(entry_col == here).astype(BF16))
        at = (found[0:1] - first) * each + found[1:2] + (crew_band_col * held).astype(F32)
        return flag(count_up((crowd, crew), 0) == at).astype(BF16)

    def first_seds(g):
        cross = dot_nt(fit[g, 0, width:used], morph_of(g, 0))
        for f in range(1, foot):
            cross = cross + dot_nt(fit[g, f, width:used], morph_of(g, f))
        old = seds[g]
        slope = dot(old.astype(BF16), gram[g]) - cross * same_t
        sed = jnp.maximum(old - slope * every_band(sed_step[g, :, 0:1]), 0.0).astype(BF16)
        return [(seds, g, sed.astype(F32))]

    def plan_move(g):
        sed = seds[g]
        bold = sed.astype(BF16)
        small = dot_nt(bold, bold)
        flat = jnp.sum(small * small, axis=1, keepdims=True).reshape(bands, size, 1)
        step = 1.0 / (jnp.sqrt(jnp.sum(flat, axis=0)) + 1.0)
        blank = jnp.zeros((span, depth - width), F32)
        right = (unit - jnp.concatenate([sed, blank], axis=1)) * every_band(step)
        right = jnp.concatenate([right, lift * (-0.1 * step)], axis=0).astype(BF16)
        left = dot_nt(eye, jnp.concatenate([sed, members], axis=0).astype(BF16)).astype(BF16)
        return [(move, g, dot(left, right).astype(BF16))]

    def moved(g, f):
        shift = dot(move[g], fit[g, f])
        return jnp.maximum(fit[g, f, 0:width].astype(F32) + shift, 0.0).astype(BF16)

    def first_morphs(g):
        return [(fit, (g, f, slice(0, width)), moved(g, f)) for f in range(foot)]

    def second_seds(g):
        total = dot_nt(fit[g, 0, 0:used], morph_of(g, 0))
        for f in range(1, foot):
            total = total + dot_nt(fit[g, f, 0:used], morph_of(g, f))
        cross = total[width:used] * same_t
        total = total[0:width] * same
        old = seds[g]
        slope = dot(old.astype(BF16), total.astype(BF16)) - cross
        sed = jnp.maximum(old - slope * every_band(sed_stepsize(total)), 0.0).astype(BF16)
        return [(seds, g, sed.astype(F32))]

    def last_models(g):
        sed = seds[g].astype(BF16)
        return [(mod, (g, f), dot(sed, morph_of(g, f)).astype(BF16)) for f in range(foot)]

    for h in range(halves):
        for k in range(len(teams)):
            give[h, k] = give_of(h, k * team)
            give_t[h, k] = give_t_of(h, k * team)

    trips = []
    for h in range(halves):
        first = h * per_half
        fetches[h][1]()
        block = jnp.zeros((crew, pixels), F32)
        for k, who in enumerate(teams):
            come = arrived[h, who].astype(F32).reshape(crowd, pixels).astype(BF16)
            block = block + dot(give[h, k], come)
        block = block.astype(BF16).reshape(per_half, foot, span, pixels)
        fit[first : first + per_half, :, width:used] = block
        over_groups(first_seds, first, per_half, 4)
        over_groups(plan_move, first, per_half, 4)
        over_groups(first_morphs, first, per_half, 4)
        over_groups(second_seds, first, per_half, 4)
        over_groups(plan_move, first, per_half, 4)
        over_groups(first_morphs, first, per_half, 4)
        over_groups(last_models, first, per_half, 4)
        models = mod[first : first + per_half].reshape(crew, pixels)
        for k, who in enumerate(teams):
            block = dot(give_t[h, k], models)
            outb[h, who] = block.reshape(team, each, pixels).astype(BF16)
        trips.append(exchange(outb.at[h], ret.at[h], back_s.at[h], back_r.at[h]))
        trips[h][0]()
        ret[h, me] = outb[h, me]

    def put_back(g, placed):
        lean = dot_nt(gather_k, seds[g].astype(BF16))
        return placed + dot(lean.astype(BF16), chosen(g))

    for h in range(halves):
        for k, who in enumerate(teams):
            pick_t[h, k] = pick_t_of(h, who)
    placed = lax.fori_loop(0, groups, put_back, jnp.zeros((comps, bands * rows), F32))
    for b in range(bands):
        sed_made[b] = placed[:, b * rows : (b + 1) * rows].astype(BF16)
    keep_sed = pltpu.make_async_copy(sed_made, sed_out, in_sem.at[0])
    keep_sed.start()

    for h in range(halves):
        trips[h][1]()
        total = jnp.zeros((stock, pixels), F32)
        for k, who in enumerate(teams):
            come = ret[h, who].astype(F32).reshape(crowd, pixels).astype(BF16)
            total = total + dot(pick_t[h, k], come)
        left = tiles if h == 0 else white
        white[...] = left[...] - total.reshape(bands, tile_rows, pixels)

    keep_white = pltpu.make_async_copy(white, white_out, in_sem.at[1])
    keep_white.start()
    squares = jnp.zeros((8, 128), F32)
    for b in range(bands):
        square = white[b] * white[b]
        for r in range(0, tile_rows, 8):
            for c in range(0, pixels, 128):
                squares = squares + square[r : r + 8, c : c + 128]

    own_row = jnp.sum(squares, axis=0, keepdims=True)
    part[...] = own_row

    def share(step, incoming):
        there = lax.rem(my + step, everyone)
        here = lax.rem(my - step + everyone, everyone) if incoming else my
        return pltpu.make_async_remote_copy(
            src_ref=part, dst_ref=parts.at[here], send_sem=sum_s.at[step],
            recv_sem=sum_r.at[step],
            device_id={"grp": lax.div(there, peers), "dev": lax.rem(there, peers)}, device_id_type=MESH,
        )

    def start_share(step, carry):
        share(step, False).start()
        return carry

    def end_share(step, carry):
        share(step, True).wait_recv()
        return carry

    def end_sent(step, carry):
        share(step, False).wait_send()
        return carry

    lax.fori_loop(1, everyone, start_share, 0)
    parts[my] = own_row
    ask_out()
    for trip in fetches + trips:
        trip[2]()
    lax.fori_loop(1, everyone, end_share, 0)
    total = jnp.sum(parts[...], axis=0)
    total = jnp.sum(jnp.sum(total, axis=1, keepdims=True), axis=0, keepdims=True)
    count_all = float(bands * tile_rows * pixels * everyone)
    scale_out[...] = jnp.broadcast_to(1.0 / jnp.sqrt(total / count_all + 1e-06), (8, 128))
    lax.fori_loop(1, everyone, end_sent, 0)
    keep_sed.wait()
    keep_white.wait()


def finish(scale, residual, sed, white_out, sed_out):
    white_out[...] = residual[...] * scale[0:1, 0:1]
    sed_out[...] = sed[...]


def on_device(pixel_tiles, blend_source, blend_slot, component_count, sed_start, morph_start):
    peers = lax.axis_size("dev")
    regions = lax.axis_size("grp")
    rows, foot = blend_source.shape
    tile_rows, bands, pixels = pixel_tiles.shape
    comps = sed_start.shape[1]
    size = math.gcd(rows, 8)
    groups = rows // size
    halves, held = plan_slots(peers, rows, foot, bands, groups)
    width = size * comps
    span = size * bands
    depth = tgt_depth(width, span)
    vmem = pl.BlockSpec(memory_space=pltpu.VMEM)
    hbm = pl.BlockSpec(memory_space=pl.ANY)
    dma = pltpu.SemaphoreType.DMA
    team = math.gcd(peers, 16)
    crowd = team * bands * held
    crew = groups // halves * foot * span
    parcel = pltpu.VMEM((halves, peers, bands * held, pixels), BF16)
    residual, sed_final, scale = pl.pallas_call(
        functools.partial(kernel, peers, regions, halves, held, size),
        out_shape=(
            jax.ShapeDtypeStruct((bands, tile_rows, pixels), F32),
            jax.ShapeDtypeStruct((bands, comps, rows), BF16),
            jax.ShapeDtypeStruct((8, 128), F32),
        ),
        in_specs=[hbm] * 6,
        out_specs=(hbm, hbm, vmem),
        scratch_shapes=[
            pltpu.VMEM((foot, rows), jnp.int32),
            pltpu.VMEM((foot, rows), jnp.int32),
            pltpu.VMEM((1, rows), jnp.int32),
            pltpu.VMEM((bands, comps, rows), BF16),
            pltpu.VMEM((bands, tile_rows, pixels), F32),
            pltpu.VMEM((bands, comps, rows), BF16),
            pltpu.VMEM((bands, tile_rows, pixels), F32),
            pltpu.VMEM((bands * tile_rows, pixels), BF16),
            pltpu.VMEM(morph_start.shape, BF16),
            pltpu.VMEM((groups, foot, depth, pixels), BF16),
            pltpu.VMEM((groups, width, width), BF16),
            pltpu.VMEM((groups, span, width), F32),
            pltpu.VMEM((groups, size, 128), F32),
            pltpu.VMEM((groups, width, depth), BF16),
            pltpu.VMEM((groups, foot, span, pixels), BF16),
            pltpu.VMEM((halves, peers // team, crew, crowd), BF16),
            pltpu.VMEM((halves, peers // team, crowd, crew), BF16),
            pltpu.VMEM((halves, peers // team, bands * tile_rows, crowd), BF16),
            pltpu.VMEM((8, 128), jnp.int32),
            pltpu.SMEM((8, 128), jnp.int32),
            pltpu.VMEM((peers, 1, 128), F32),
            pltpu.VMEM((peers, 1, 128), F32),
            parcel,
            parcel,
            parcel,
            parcel,
            pltpu.VMEM((1, 128), F32),
            pltpu.VMEM((peers * regions, 1, 128), F32),
            dma((7,)),
            dma((peers,)),
            dma((peers,)),
            dma((halves, peers)),
            dma((halves, peers)),
            dma((halves, peers)),
            dma((halves, peers)),
            dma((peers * regions,)),
            dma((peers * regions,)),
        ],
        compiler_params=pltpu.CompilerParams(
            collective_id=0, has_side_effects=True, vmem_limit_bytes=40 * 1024 * 1024
        ),
    )(
        *[
            pltpu.with_memory_space_constraint(given, pltpu.HBM)
            for given in (
                jnp.transpose(pixel_tiles, (1, 0, 2)),
                jnp.transpose(blend_source),
                jnp.transpose(blend_slot),
                component_count.reshape(1, rows),
                jnp.transpose(sed_start, (2, 1, 0)),
                morph_start,
            )
        ]
    )
    white, sed_final = pl.pallas_call(
        finish,
        out_shape=(
            jax.ShapeDtypeStruct((bands, tile_rows, pixels), F32),
            jax.ShapeDtypeStruct((bands, comps, rows), BF16),
        ),
        in_specs=[vmem, vmem, vmem],
        out_specs=(vmem, vmem),
        compiler_params=pltpu.CompilerParams(vmem_limit_bytes=8 * 1024 * 1024),
    )(scale, residual, sed_final)
    return jnp.transpose(white, (1, 0, 2)), jnp.transpose(sed_final, (2, 1, 0))


def solution(mesh):
    placed = (
        P(("grp", "dev"), None, None),
        P(("grp", "dev"), None),
        P(("grp", "dev"), None),
        P(("grp", "dev")),
        P(("grp", "dev"), None, None),
        P(("grp", "dev"), None, None, None),
    )
    return jax.shard_map(
        on_device,
        mesh=mesh,
        in_specs=placed,
        out_specs=(P(("grp", "dev"), None, None), P(("grp", "dev"), None, None)),
        check_vma=False,
    )
```

```python
import functools
import math

import jax
import jax.numpy as jnp
from jax import lax
from jax.experimental import pallas as pl
from jax.experimental.pallas import tpu as pltpu
from jax.sharding import PartitionSpec as P

F32 = jnp.float32
BF16 = jnp.bfloat16
MESH = pl.DeviceIdType.MESH


def dot(a, b):
    return jnp.dot(a, b, preferred_element_type=F32)


def dot_nt(a, b):
    return lax.dot_general(a, b, (((1,), (1,)), ((), ())), preferred_element_type=F32)


def iota(shape, dimension):
    return lax.broadcasted_iota(jnp.int32, shape, dimension)


def count_up(shape, dimension):
    return iota(shape, dimension).astype(F32)


def split_row(shape, dimension, width):
    place = iota(shape, dimension)
    out = jnp.zeros(shape, jnp.int32)
    for cut in range(width, shape[dimension], width):
        out = out + (place >= cut).astype(jnp.int32)
    return out, place - out * width


def flag(condition):
    return condition.astype(F32)


def lanes_of(*parts):
    return parts[0] if len(parts) == 1 else jnp.concatenate(parts, axis=1)


def rows_of(*parts):
    return parts[0] if len(parts) == 1 else jnp.concatenate(parts, axis=0)


def tgt_depth(width, span):
    return (width + span) // 16 * 16 + 16


def plan_slots(peers, rows, foot, bands, groups):
    entries = rows * foot
    capacity = max(2, (entries + peers - 1) // peers)
    even = foot == 2 and peers * capacity == entries and capacity % 4 == 0
    halves = 2 if even and groups % 2 == 0 and entries == 128 else 1
    held = capacity // halves
    while held * bands % 8:
        held = held + 1
    return halves, held


def partners(col, row, before, after):
    alike = flag(col == row)
    rank_col = jnp.sum(alike * before, axis=1, keepdims=True)
    rank_row = jnp.sum(alike * after, axis=0, keepdims=True)
    level = flag(jnp.floor(rank_col * 0.5) == jnp.floor(rank_row * 0.5))
    return alike * level * (before + after)


def halve(source_col, source_row, n):
    entries = 2 * n
    before = flag(iota((entries, entries), 1) < iota((entries, entries), 0))
    after = flag(iota((entries, entries), 1) > iota((entries, entries), 0))
    pair = partners(source_col, source_row, before, after)
    step = rows_of(pair[n:], pair[:n]).astype(BF16)
    least = count_up((entries, entries), 0)
    reach = 1
    while reach < n:
        both = dot(step, lanes_of(step, least.astype(BF16)))
        least = jnp.minimum(least, both[:, entries:])
        step = both[:, :entries].astype(BF16)
        reach = reach * 2
    tail = (least[:n] < least[n:])[:, 0:1]
    tail_col = jnp.where(tail, source_col[:n], source_col[n:])
    head_col = jnp.where(tail, source_col[n:], source_col[:n])
    lane = iota((n, 128), 1)
    turned = jnp.transpose(jnp.where(lane == 0, tail_col, jnp.where(lane == 1, head_col, 0.0)))
    before = before[:n, :n]
    after = after[:n, :n]
    tails = partners(tail_col, turned[0:1], before, after).astype(BF16)
    heads = partners(head_col, turned[1:2], before, after).astype(BF16)
    step = dot(tails, heads).astype(BF16)
    least = count_up((n, n), 0)
    reach = 1
    while reach < n // 2:
        least = jnp.minimum(least, dot(step, least.astype(BF16)))
        step = dot(step, step).astype(BF16)
        reach = reach * 2
    return flag(least >= dot(tails, least.astype(BF16)))


def kernel(
    peers, regions, halves, held, size,
    tiles_hbm, source_hbm, slot_hbm, count_hbm, sed_hbm, morph_hbm, white_out, sed_out, scale_out, source, slot, count, sed0,
    white, sed_made, tiles, tiles_b, morph_in, fit, gram, seds, sed_step, move, mod, give, give_t, pick_t, order_v, order_s, req, wanted, send, arrived, outb, ret, part, parts,
    in_sem, ask_s, ask_r, put_s, put_r, back_s, back_r, sum_s, sum_r,
):
    bands, tile_rows, pixels = tiles.shape
    foot, rows = source.shape
    comps = sed0.shape[1]
    groups = rows // size
    per_half = groups // halves
    me = lax.axis_index("dev")
    everyone = peers * regions
    my = lax.axis_index("grp") * peers + me
    small = [
        pltpu.make_async_copy(given, kept, in_sem.at[3 + i])
        for i, (given, kept) in enumerate(
            ((source_hbm, source), (slot_hbm, slot), (count_hbm, count), (sed_hbm, sed0))
        )
    ]
    for copy in small:
        copy.start()
    load_tiles = pltpu.make_async_copy(tiles_hbm, tiles, in_sem.at[0])
    load_tiles.start()
    load = pltpu.make_async_copy(morph_hbm, morph_in, in_sem.at[1])
    load.start()
    barrier = pltpu.get_barrier_semaphore()

    def greet(step, carry):
        other = lax.rem(my + step, everyone)
        pl.semaphore_signal(
            barrier, inc=1, device_id={"grp": lax.div(other, peers), "dev": lax.rem(other, peers)},
            device_id_type=MESH,
        )
        return carry

    lax.fori_loop(1, everyone, greet, 0)

    small[0].wait()
    small[1].wait()
    entries = foot * rows
    source_row = lanes_of(*[source[f : f + 1, :] for f in range(foot)]).astype(F32)
    slot_row = lanes_of(*[slot[f : f + 1, :] for f in range(foot)]).astype(F32)
    turned = jnp.transpose(rows_of(source_row, slot_row, jnp.zeros((6, entries), F32)))
    source_col = turned[:, 0:1]
    slot_col = turned[:, 1:2]
    before = flag(iota((entries, entries), 1) < iota((entries, entries), 0))
    after = flag(iota((entries, entries), 1) > iota((entries, entries), 0))
    alike = flag(source_col == source_row)
    if halves == 2:
        half = halve(source_col, source_row, rows)
        half_col = half[:, 0:1]
        half_row = jnp.transpose(lanes_of(half, half))[0:1]
        alone = flag(half_col == half_row)
        base = rows // 2
        pos_col = half_col * base + jnp.sum(alone * before[:rows, :rows], axis=1, keepdims=True)
        pos_row = half_row * base + jnp.sum(alone * after[:rows, :rows], axis=0, keepdims=True)
        both_col = rows_of(half_col, half_col)
        both_row = lanes_of(half_row, half_row)
        alike = alike * flag(both_col == both_row)
        rank_col = jnp.sum(alike * before, axis=1, keepdims=True)
        rank_row = jnp.sum(alike * after, axis=0, keepdims=True)
        lane_col = both_col * held + rank_col
    else:
        pos_col = count_up((rows, 1), 0)
        pos_row = count_up((1, rows), 1)
        rank_col = jnp.sum(alike * before, axis=1, keepdims=True)
        rank_row = jnp.sum(alike * after, axis=0, keepdims=True)
        lane_col = rank_col
    named = flag(count_up((peers, entries), 0) == source_row)
    asked = flag(count_up((entries, 128), 1) == lane_col) * (slot_col + 1.0)
    req[...] = dot(named.astype(BF16), asked.astype(BF16)).reshape(peers, 1, 128)
    pl.semaphore_wait(barrier, everyone - 1)

    planes = 4 if peers % 4 == 0 else 1
    deck = peers // planes
    level = lax.div(me, deck)
    spot = lax.rem(me, deck)
    upper = lax.div(level, 2)
    if planes == 4:
        decks = [2 - upper, 3 - 3 * upper, 4 * upper + 1 - level, level]
    else:
        decks = [level]

    def member(c, j):
        return decks[c] * deck + lax.rem(spot + j, deck)

    def exchange(src, dst, send_sem, recv_sem):
        def copy(there, here):
            return pltpu.make_async_remote_copy(
                src_ref=src.at[there], dst_ref=dst.at[here],
                send_sem=send_sem.at[there], recv_sem=recv_sem.at[here],
                device_id={"dev": there}, device_id_type=MESH,
            )

        def each_of(act, classes):
            for c in classes:
                def body(j, carry, c=c):
                    act(member(c, j))
                    return carry

                lax.fori_loop(1 if c == planes - 1 else 0, deck, body, 0)

        def start(classes=range(planes)):
            each_of(lambda there: copy(there, me).start(), classes)

        def wait_in(classes=range(planes)):
            each_of(lambda here: copy(here, here).wait_recv(), classes)

        def wait_out(classes=range(planes)):
            each_of(lambda there: copy(there, me).wait_send(), classes)

        return start, wait_in, wait_out

    ask, ask_in, ask_out = exchange(req, wanted, ask_s, ask_r)
    ask()
    wanted[me] = req[me]

    order = jnp.sum(flag(count_up((rows, 128), 1) == pos_col) * count_up((rows, 128), 0), axis=0, keepdims=True)
    order = jnp.minimum(order, float(rows - 1))
    order_v[...] = jnp.broadcast_to(order, (8, 128)).astype(jnp.int32)
    to_scalars = pltpu.make_async_copy(order_v, order_s, in_sem.at[2])
    to_scalars.start()

    small[2].wait()
    small[3].wait()
    width = size * comps
    span = size * bands
    used = width + span
    depth = tgt_depth(width, span)
    blend_row, comp_row = split_row((width, 1), 0, comps)
    blend_col, comp_col = split_row((1, width), 1, comps)
    band_row, member_row = split_row((span, 1), 0, size)
    same = flag(blend_row == blend_col)
    same_t = flag(member_row == blend_col)
    members = flag(iota((size, width), 0) == blend_col)
    unit = flag(iota((span, depth), 0) + width == iota((span, depth), 1))
    lift = flag(iota((size, depth), 1) == used)
    eye = flag(iota((width, width), 0) == iota((width, width), 1)).astype(BF16)
    gather_k = flag(iota((comps, width), 0) == comp_col).astype(BF16)
    sed_all = jnp.concatenate([sed0[b].astype(F32) for b in range(bands)], axis=1).astype(BF16)
    band_of, _ = split_row((1, bands * rows), 1, rows)
    pos_of = lanes_of(*[pos_row] * bands)
    counts = jnp.broadcast_to(count[...], (8, rows)).astype(F32).astype(BF16)

    def chosen(g):
        hit = (band_of == band_row) & (pos_of == (g * size + member_row).astype(F32))
        return flag(hit).astype(BF16)

    def every_band(column):
        return jnp.concatenate([column] * bands, axis=0)

    def sed_stepsize(total):
        flat = jnp.sum(total * total, axis=0, keepdims=True)
        return 1.0 / (jnp.sqrt(jnp.sum(members * flat, axis=1, keepdims=True)) + 1.0)

    def wide(column):
        return jnp.broadcast_to(column, (column.shape[0], 128))

    def over_groups(body, first, number, pair):
        pair = math.gcd(number, pair)

        def some(j, carry):
            stores = []
            for k in range(pair):
                stores = stores + body(first + j * pair + k)
            for ref, index, value in stores:
                ref[index] = value
            return carry

        lax.fori_loop(0, number // pair, some, 0)

    to_scalars.wait()
    load.wait()

    def begin(g):
        mine = pos_row == (g * size + blend_row).astype(F32)
        kept = jnp.sum(jnp.where(mine, count[...].astype(F32), 0.0), axis=1, keepdims=True)
        active = flag(comp_row.astype(F32) < kept)
        owner = flag(pos_col == (g * size + blend_col).astype(F32)).astype(BF16)
        active_t = flag(comp_col.astype(F32) < dot(counts, owner)[0:1])
        first = dot_nt(chosen(g), sed_all)
        stores = [(seds, g, dot(first.astype(BF16), gather_k) * same_t * active_t)]
        tail = flag(iota((depth - used, pixels), 0) == 0).astype(BF16)
        places = [jnp.clip(order_s[0, g * size + m], 0, rows - 1) for m in range(size)]
        for f in range(foot):
            whole = rows_of(*[morph_in[place, f].astype(F32) for place in places])
            stores.append((fit, (g, f, slice(0, width)), (whole * active).astype(BF16)))
            stores.append((fit, (g, f, slice(used, depth)), tail))
        return stores

    over_groups(begin, 0, groups, 2)
    load_tiles.wait()
    tiles_b[...] = tiles[...].reshape(bands * tile_rows, pixels).astype(BF16)

    team = math.gcd(peers, 16)
    each = bands * held
    crowd = team * each
    stock = bands * tile_rows
    teams = [slice(k, k + team) for k in range(0, peers, team)]
    peer_col = split_row((1, crowd), 1, each)[0]
    seat_band_col, seat_rank_col = split_row((1, crowd), 1, held)
    seat_band_col = seat_band_col - peer_col * bands

    ranks = deck * each
    asker_row, seat_rank_row = split_row((ranks, 1), 0, held)
    seat_band_row = asker_row - split_row((ranks, 1), 0, each)[0] * bands

    def pick_of(h, c):
        lines = rows_of(*[jnp.broadcast_to(wanted[member(c, j)], (each, 128)) for j in range(deck)])
        seat = flag(iota((ranks, 128), 1) == h * held + seat_rank_row)
        tile = jnp.sum(lines * seat, axis=1, keepdims=True)
        at = jnp.where(tile > 0.0, tile - 1.0 + (seat_band_row * tile_rows).astype(F32), -1.0)
        return flag(count_up((ranks, stock), 1) == at).astype(BF16)

    def pick_t_of(h, who):
        lines = wanted[who].reshape(team, 128).astype(BF16)
        seat = flag(iota((128, crowd), 0) == h * held + seat_rank_col).astype(BF16)
        tile = dot(lines, seat) * flag(iota((team, crowd), 0) == peer_col)
        tile = jnp.sum(tile, axis=0, keepdims=True)
        at = jnp.where(tile > 0.0, tile - 1.0 + (seat_band_col * tile_rows).astype(F32), -1.0)
        return flag(count_up((stock, crowd), 0) == at).astype(BF16)

    fetches = [
        exchange(send.at[h], arrived.at[h], put_s.at[h], put_r.at[h]) for h in range(halves)
    ]
    for h in range(halves):
        for c in range(planes):
            if h == 0:
                ask_in([c])
            block = dot(pick_of(h, c), tiles_b[...]).astype(BF16)
            for j in range(deck):
                send[h, member(c, j)] = block[j * each : (j + 1) * each]
            fetches[h][0]([c])
        arrived[h, me] = send[h, me]

    def morph_of(g, f):
        return fit[g, f, 0:width]

    def first_gram(g):
        total = dot_nt(morph_of(g, 0), morph_of(g, 0))
        for f in range(1, foot):
            total = total + dot_nt(morph_of(g, f), morph_of(g, f))
        total = total * same
        return [(gram, g, total.astype(BF16)), (sed_step, g, wide(sed_stepsize(total)))]

    over_groups(first_gram, 0, groups, 4)

    crew = per_half * foot * span
    crew_row, crew_band_row = split_row((crew, 1), 0, span)
    crew_band_row, crew_member_row = split_row((crew, 1), 0, size)
    crew_band_row = crew_band_row - crew_row * bands
    crew_col, _ = split_row((1, crew), 1, span)
    crew_band_col, crew_member_col = split_row((1, crew), 1, size)
    crew_band_col = crew_band_col - crew_col * bands
    group_row = split_row((crew, 1), 0, foot * span)[0]
    group_col = split_row((1, crew), 1, foot * span)[0]
    foot_row = crew_row - group_row * foot
    foot_col = crew_col - group_col * foot
    entry_row = lanes_of(*[pos_row + f * rows for f in range(foot)])
    entry_col = rows_of(*[pos_col + f * rows for f in range(foot)])
    facts = lanes_of(
        jnp.broadcast_to(source_col, (entries, 128)), jnp.broadcast_to(rank_col, (entries, 128))
    ).astype(BF16)
    facts_t = rows_of(source_row, rank_row, jnp.zeros((6, entries), F32)).astype(BF16)

    def give_of(h, first):
        here = ((h * per_half + group_row) * size + crew_member_row + foot_row * rows).astype(F32)
        found = dot(flag(here == entry_row).astype(BF16), facts)
        at = (found[:, 0:1] - first) * each + found[:, 128:129] + (crew_band_row * held).astype(F32)
        return flag(count_up((crew, crowd), 1) == at).astype(BF16)

    def give_t_of(h, first):
        here = ((h * per_half + group_col) * size + crew_member_col + foot_col * rows).astype(F32)
        found = dot(facts_t, flag(entry_col == here).astype(BF16))
        at = (found[0:1] - first) * each + found[1:2] + (crew_band_col * held).astype(F32)
        return flag(count_up((crowd, crew), 0) == at).astype(BF16)

    def first_seds(g):
        cross = dot_nt(fit[g, 0, width:used], morph_of(g, 0))
        for f in range(1, foot):
            cross = cross + dot_nt(fit[g, f, width:used], morph_of(g, f))
        old = seds[g]
        slope = dot(old.astype(BF16), gram[g]) - cross * same_t
        sed = jnp.maximum(old - slope * every_band(sed_step[g, :, 0:1]), 0.0).astype(BF16)
        return [(seds, g, sed.astype(F32))]

    def plan_move(g):
        sed = seds[g]
        bold = sed.astype(BF16)
        small = dot_nt(bold, bold)
        flat = jnp.sum(small * small, axis=1, keepdims=True).reshape(bands, size, 1)
        step = 1.0 / (jnp.sqrt(jnp.sum(flat, axis=0)) + 1.0)
        blank = jnp.zeros((span, depth - width), F32)
        right = (unit - jnp.concatenate([sed, blank], axis=1)) * every_band(step)
        right = jnp.concatenate([right, lift * (-0.1 * step)], axis=0).astype(BF16)
        left = dot_nt(eye, jnp.concatenate([sed, members], axis=0).astype(BF16)).astype(BF16)
        return [(move, g, dot(left, right).astype(BF16))]

    def moved(g, f):
        shift = dot(move[g], fit[g, f])
        return jnp.maximum(fit[g, f, 0:width].astype(F32) + shift, 0.0).astype(BF16)

    def first_morphs(g):
        return [(fit, (g, f, slice(0, width)), moved(g, f)) for f in range(foot)]

    def second_seds(g):
        total = dot_nt(fit[g, 0, 0:used], morph_of(g, 0))
        for f in range(1, foot):
            total = total + dot_nt(fit[g, f, 0:used], morph_of(g, f))
        cross = total[width:used] * same_t
        total = total[0:width] * same
        old = seds[g]
        slope = dot(old.astype(BF16), total.astype(BF16)) - cross
        sed = jnp.maximum(old - slope * every_band(sed_stepsize(total)), 0.0).astype(BF16)
        return [(seds, g, sed.astype(F32))]

    def last_models(g):
        sed = seds[g].astype(BF16)
        return [(mod, (g, f), dot(sed, morph_of(g, f)).astype(BF16)) for f in range(foot)]

    for h in range(halves):
        for k in range(len(teams)):
            give[h, k] = give_of(h, k * team)
            give_t[h, k] = give_t_of(h, k * team)

    trips = []
    for h in range(halves):
        first = h * per_half
        fetches[h][1]()
        block = jnp.zeros((crew, pixels), F32)
        for k, who in enumerate(teams):
            come = arrived[h, who].astype(F32).reshape(crowd, pixels).astype(BF16)
            block = block + dot(give[h, k], come)
        block = block.astype(BF16).reshape(per_half, foot, span, pixels)
        fit[first : first + per_half, :, width:used] = block
        over_groups(first_seds, first, per_half, 4)
        over_groups(plan_move, first, per_half, 4)
        over_groups(first_morphs, first, per_half, 4)
        over_groups(second_seds, first, per_half, 4)
        over_groups(plan_move, first, per_half, 4)
        over_groups(first_morphs, first, per_half, 4)
        over_groups(last_models, first, per_half, 4)
        models = mod[first : first + per_half].reshape(crew, pixels)
        for k, who in enumerate(teams):
            block = dot(give_t[h, k], models)
            outb[h, who] = block.reshape(team, each, pixels).astype(BF16)
        trips.append(exchange(outb.at[h], ret.at[h], back_s.at[h], back_r.at[h]))
        trips[h][0]()
        ret[h, me] = outb[h, me]

    def put_back(g, placed):
        lean = dot_nt(gather_k, seds[g].astype(BF16))
        return placed + dot(lean.astype(BF16), chosen(g))

    for h in range(halves):
        for k, who in enumerate(teams):
            pick_t[h, k] = pick_t_of(h, who)
    placed = lax.fori_loop(0, groups, put_back, jnp.zeros((comps, bands * rows), F32))
    for b in range(bands):
        sed_made[b] = placed[:, b * rows : (b + 1) * rows].astype(BF16)
    keep_sed = pltpu.make_async_copy(sed_made, sed_out, in_sem.at[0])
    keep_sed.start()

    for h in range(halves):
        trips[h][1]()
        total = jnp.zeros((stock, pixels), F32)
        for k, who in enumerate(teams):
            come = ret[h, who].astype(F32).reshape(crowd, pixels).astype(BF16)
            total = total + dot(pick_t[h, k], come)
        left = tiles if h == 0 else white
        white[...] = left[...] - total.reshape(bands, tile_rows, pixels)

    keep_white = pltpu.make_async_copy(white, white_out, in_sem.at[1])
    keep_white.start()
    squares = jnp.zeros((8, 128), F32)
    for b in range(bands):
        square = white[b] * white[b]
        for r in range(0, tile_rows, 8):
            for c in range(0, pixels, 128):
                squares = squares + square[r : r + 8, c : c + 128]

    own_row = jnp.sum(squares, axis=0, keepdims=True)
    part[...] = own_row

    place_of = me * regions + lax.axis_index("grp")

    def share(step, incoming):
        other = step + (step >= place_of).astype(jnp.int32)
        return pltpu.make_async_remote_copy(
            src_ref=part, dst_ref=parts.at[other if incoming else place_of], send_sem=sum_s.at[other],
            recv_sem=sum_r.at[other if incoming else place_of],
            device_id={"grp": lax.rem(other, regions), "dev": lax.div(other, regions)}, device_id_type=MESH,
        )

    def start_share(step, carry):
        share(step, False).start()
        return carry

    def end_share(step, carry):
        share(step, True).wait_recv()
        return carry

    def end_sent(step, carry):
        share(step, False).wait_send()
        return carry

    lax.fori_loop(0, everyone - 1, start_share, 0)
    parts[place_of] = own_row
    ask_out()
    for trip in fetches + trips:
        trip[2]()
    lax.fori_loop(0, everyone - 1, end_share, 0)
    total = jnp.sum(parts[...], axis=0)
    total = jnp.sum(jnp.sum(total, axis=1, keepdims=True), axis=0, keepdims=True)
    count_all = float(bands * tile_rows * pixels * everyone)
    scale_out[...] = jnp.broadcast_to(1.0 / jnp.sqrt(total / count_all + 1e-06), (8, 128))
    lax.fori_loop(0, everyone - 1, end_sent, 0)
    keep_sed.wait()
    keep_white.wait()


def finish(scale, residual, sed, white_out, sed_out):
    white_out[...] = residual[...] * scale[0:1, 0:1]
    sed_out[...] = sed[...]


def on_device(pixel_tiles, blend_source, blend_slot, component_count, sed_start, morph_start):
    peers = lax.axis_size("dev")
    regions = lax.axis_size("grp")
    rows, foot = blend_source.shape
    tile_rows, bands, pixels = pixel_tiles.shape
    comps = sed_start.shape[1]
    size = math.gcd(rows, 8)
    groups = rows // size
    halves, held = plan_slots(peers, rows, foot, bands, groups)
    width = size * comps
    span = size * bands
    depth = tgt_depth(width, span)
    vmem = pl.BlockSpec(memory_space=pltpu.VMEM)
    hbm = pl.BlockSpec(memory_space=pl.ANY)
    dma = pltpu.SemaphoreType.DMA
    team = math.gcd(peers, 16)
    crowd = team * bands * held
    crew = groups // halves * foot * span
    parcel = pltpu.VMEM((halves, peers, bands * held, pixels), BF16)
    residual, sed_final, scale = pl.pallas_call(
        functools.partial(kernel, peers, regions, halves, held, size),
        out_shape=(
            jax.ShapeDtypeStruct((bands, tile_rows, pixels), F32),
            jax.ShapeDtypeStruct((bands, comps, rows), BF16),
            jax.ShapeDtypeStruct((8, 128), F32),
        ),
        in_specs=[hbm] * 6,
        out_specs=(hbm, hbm, vmem),
        scratch_shapes=[
            pltpu.VMEM((foot, rows), jnp.int32),
            pltpu.VMEM((foot, rows), jnp.int32),
            pltpu.VMEM((1, rows), jnp.int32),
            pltpu.VMEM((bands, comps, rows), BF16),
            pltpu.VMEM((bands, tile_rows, pixels), F32),
            pltpu.VMEM((bands, comps, rows), BF16),
            pltpu.VMEM((bands, tile_rows, pixels), F32),
            pltpu.VMEM((bands * tile_rows, pixels), BF16),
            pltpu.VMEM(morph_start.shape, BF16),
            pltpu.VMEM((groups, foot, depth, pixels), BF16),
            pltpu.VMEM((groups, width, width), BF16),
            pltpu.VMEM((groups, span, width), F32),
            pltpu.VMEM((groups, size, 128), F32),
            pltpu.VMEM((groups, width, depth), BF16),
            pltpu.VMEM((groups, foot, span, pixels), BF16),
            pltpu.VMEM((halves, peers // team, crew, crowd), BF16),
            pltpu.VMEM((halves, peers // team, crowd, crew), BF16),
            pltpu.VMEM((halves, peers // team, bands * tile_rows, crowd), BF16),
            pltpu.VMEM((8, 128), jnp.int32),
            pltpu.SMEM((8, 128), jnp.int32),
            pltpu.VMEM((peers, 1, 128), F32),
            pltpu.VMEM((peers, 1, 128), F32),
            parcel,
            parcel,
            parcel,
            parcel,
            pltpu.VMEM((1, 128), F32),
            pltpu.VMEM((peers * regions, 1, 128), F32),
            dma((7,)),
            dma((peers,)),
            dma((peers,)),
            dma((halves, peers)),
            dma((halves, peers)),
            dma((halves, peers)),
            dma((halves, peers)),
            dma((peers * regions,)),
            dma((peers * regions,)),
        ],
        compiler_params=pltpu.CompilerParams(
            collective_id=0, has_side_effects=True, vmem_limit_bytes=40 * 1024 * 1024
        ),
    )(
        *[
            pltpu.with_memory_space_constraint(given, pltpu.HBM)
            for given in (
                jnp.transpose(pixel_tiles, (1, 0, 2)),
                jnp.transpose(blend_source),
                jnp.transpose(blend_slot),
                component_count.reshape(1, rows),
                jnp.transpose(sed_start, (2, 1, 0)),
                morph_start,
            )
        ]
    )
    white, sed_final = pl.pallas_call(
        finish,
        out_shape=(
            jax.ShapeDtypeStruct((bands, tile_rows, pixels), F32),
            jax.ShapeDtypeStruct((bands, comps, rows), BF16),
        ),
        in_specs=[vmem, vmem, vmem],
        out_specs=(vmem, vmem),
        compiler_params=pltpu.CompilerParams(vmem_limit_bytes=8 * 1024 * 1024),
    )(scale, residual, sed_final)
    return jnp.transpose(white, (1, 0, 2)), jnp.transpose(sed_final, (2, 1, 0))


def solution(mesh):
    placed = (
        P(("grp", "dev"), None, None),
        P(("grp", "dev"), None),
        P(("grp", "dev"), None),
        P(("grp", "dev")),
        P(("grp", "dev"), None, None),
        P(("grp", "dev"), None, None, None),
    )
    return jax.shard_map(
        on_device,
        mesh=mesh,
        in_specs=placed,
        out_specs=(P(("grp", "dev"), None, None), P(("grp", "dev"), None, None)),
        check_vma=False,
    )
```

```python
import functools
import math

import jax
import jax.numpy as jnp
from jax import lax
from jax.experimental import pallas as pl
from jax.experimental.pallas import tpu as pltpu
from jax.sharding import PartitionSpec as P

F32 = jnp.float32
BF16 = jnp.bfloat16
MESH = pl.DeviceIdType.MESH


def dot(a, b):
    return jnp.dot(a, b, preferred_element_type=F32)


def dot_nt(a, b):
    return lax.dot_general(a, b, (((1,), (1,)), ((), ())), preferred_element_type=F32)


def iota(shape, dimension):
    return lax.broadcasted_iota(jnp.int32, shape, dimension)


def count_up(shape, dimension):
    return iota(shape, dimension).astype(F32)


def split_row(shape, dimension, width):
    place = iota(shape, dimension)
    out = jnp.zeros(shape, jnp.int32)
    for cut in range(width, shape[dimension], width):
        out = out + (place >= cut).astype(jnp.int32)
    return out, place - out * width


def flag(condition):
    return condition.astype(F32)


def lanes_of(*parts):
    return parts[0] if len(parts) == 1 else jnp.concatenate(parts, axis=1)


def rows_of(*parts):
    return parts[0] if len(parts) == 1 else jnp.concatenate(parts, axis=0)


def tgt_depth(width, span):
    return (width + span) // 16 * 16 + 16


def plan_slots(peers, rows, foot, bands, groups):
    entries = rows * foot
    capacity = max(2, (entries + peers - 1) // peers)
    even = foot == 2 and peers * capacity == entries and capacity % 4 == 0
    halves = 2 if even and groups % 2 == 0 and entries == 128 else 1
    held = capacity // halves
    while held * bands % 8:
        held = held + 1
    return halves, held


def turn(*lines):
    n = lines[0].shape[1]
    return jnp.transpose(rows_of(*lines, jnp.zeros((8 - len(lines), n), F32)))


def partners(col, row):
    shape = (col.shape[0], row.shape[1])
    here, there = iota(shape, 0), iota(shape, 1)
    alike = flag(col == row)
    rank_col = jnp.sum(alike * flag(there < here), axis=1, keepdims=True)
    rank_row = jnp.sum(alike * flag(there > here), axis=0, keepdims=True)
    level = flag(jnp.floor(rank_col * 0.5) == jnp.floor(rank_row * 0.5))
    pair = alike * level * flag(here != there)
    found = jnp.sum(pair * here.astype(F32), axis=0, keepdims=True)
    return jnp.broadcast_to(found, (8, shape[1])).astype(jnp.int32)


def follow(values, at):
    return jnp.take_along_axis(values, at, axis=1)


def lowest(step, length):
    least = iota(step.shape, 1)
    reach = 1
    while reach < length:
        least = jnp.minimum(least, follow(least, step))
        step = follow(step, step)
        reach = reach * 2
    return least


def halve(source_col, source_row, n):
    def swap(values):
        return jnp.concatenate([values[:, n:], values[:, :n]], axis=1)

    least = lowest(swap(partners(source_col, source_row)), n)
    tail = (least < swap(least))[0:1]
    other_row = swap(source_row)
    tail_row = jnp.where(tail, source_row, other_row)
    head_row = jnp.where(tail, other_row, source_row)
    turned = turn(tail_row, head_row)[:n]
    lane = iota((n, 2 * n), 1)
    tails = partners(turned[:, 0:1], jnp.where(lane[0:1] < n, tail_row, -1.0))
    heads = partners(turned[:, 1:2], jnp.where(lane[0:1] < n, head_row, -1.0))
    least = lowest(follow(heads, tails), n // 2)
    return flag(least >= follow(least, tails))[0:1]


def kernel(
    peers, regions, halves, held, size,
    tiles_hbm, source_hbm, slot_hbm, count_hbm, sed_hbm, morph_hbm, white_out, sed_out, scale_out, scale_made, source, slot, count, sed0,
    white, sed_made, tiles, tiles_b, morph_in, fit, gram, seds, sed_step, move, mod, give, give_t, pick_t, order_v, order_s, req, wanted, send, arrived, outb, ret, part, parts,
    in_sem, ask_s, ask_r, put_s, put_r, back_s, back_r, sum_s, sum_r,
):
    bands, tile_rows, pixels = tiles.shape
    foot, rows = source.shape
    comps = sed0.shape[1]
    groups = rows // size
    per_half = groups // halves
    me = lax.axis_index("dev")
    everyone = peers * regions
    my = lax.axis_index("grp") * peers + me
    small = [
        pltpu.make_async_copy(given, kept, in_sem.at[3 + i])
        for i, (given, kept) in enumerate(
            ((source_hbm, source), (slot_hbm, slot), (count_hbm, count), (sed_hbm, sed0))
        )
    ]
    for copy in small:
        copy.start()
    load_tiles = pltpu.make_async_copy(tiles_hbm, tiles, in_sem.at[0])
    load_tiles.start()
    load = pltpu.make_async_copy(morph_hbm, morph_in, in_sem.at[1])
    load.start()
    barrier = pltpu.get_barrier_semaphore()

    def greet(step, carry):
        other = lax.rem(my + step, everyone)
        pl.semaphore_signal(
            barrier, inc=1, device_id={"grp": lax.div(other, peers), "dev": lax.rem(other, peers)},
            device_id_type=MESH,
        )
        return carry

    lax.fori_loop(1, everyone, greet, 0)

    small[0].wait()
    small[1].wait()
    entries = foot * rows
    source_row = lanes_of(*[source[f : f + 1, :] for f in range(foot)]).astype(F32)
    slot_row = lanes_of(*[slot[f : f + 1, :] for f in range(foot)]).astype(F32)
    turned = turn(source_row, slot_row)
    source_col = turned[:, 0:1]
    slot_col = turned[:, 1:2]
    before = flag(iota((entries, entries), 1) < iota((entries, entries), 0))
    after = flag(iota((entries, entries), 1) > iota((entries, entries), 0))
    alike = flag(source_col == source_row)
    if halves == 2:
        half = halve(source_col, source_row, rows)
        half_col = turn(half)[:rows, 0:1]
        half_row = half[:, :rows]
        alone = flag(half_col == half_row)
        base = rows // 2
        pos_col = half_col * base + jnp.sum(alone * before[:rows, :rows], axis=1, keepdims=True)
        pos_row = half_row * base + jnp.sum(alone * after[:rows, :rows], axis=0, keepdims=True)
        both_col = rows_of(half_col, half_col)
        both_row = lanes_of(half_row, half_row)
        alike = alike * flag(both_col == both_row)
        rank_col = jnp.sum(alike * before, axis=1, keepdims=True)
        rank_row = jnp.sum(alike * after, axis=0, keepdims=True)
        lane_col = both_col * held + rank_col
    else:
        pos_col = count_up((rows, 1), 0)
        pos_row = count_up((1, rows), 1)
        rank_col = jnp.sum(alike * before, axis=1, keepdims=True)
        rank_row = jnp.sum(alike * after, axis=0, keepdims=True)
        lane_col = rank_col
    named = flag(count_up((peers, entries), 0) == source_row)
    asked = flag(count_up((entries, 128), 1) == lane_col) * (slot_col + 1.0)
    req[...] = dot(named.astype(BF16), asked.astype(BF16)).reshape(peers, 1, 128)
    pl.semaphore_wait(barrier, everyone - 1)

    planes = 4 if peers % 4 == 0 else 1
    deck = peers // planes
    level = lax.div(me, deck)
    spot = lax.rem(me, deck)
    upper = lax.div(level, 2)
    if planes == 4:
        decks = [2 - upper, 3 - 3 * upper, 4 * upper + 1 - level, level]
    else:
        decks = [level]

    def member(c, j):
        return decks[c] * deck + lax.rem(spot + j, deck)

    def exchange(src, dst, send_sem, recv_sem):
        def copy(from_here, to_there, there=me):
            return pltpu.make_async_remote_copy(
                src_ref=src.at[from_here], dst_ref=dst.at[to_there], send_sem=send_sem,
                recv_sem=recv_sem, device_id={"dev": there}, device_id_type=MESH,
            )

        def start(c):
            def body(j, carry):
                there = member(c, j)
                copy(there, me, there).start()
                return carry

            lax.fori_loop(1 if c == planes - 1 else 0, deck, body, 0)

        others = pl.ds(0, peers - 1)
        return start, copy(others, others).wait_recv, copy(others, others).wait_send

    def asking(c, j):
        there = member(c, j)
        return pltpu.make_async_remote_copy(
            src_ref=req.at[there], dst_ref=wanted.at[me], send_sem=ask_s.at[c],
            recv_sem=ask_r.at[level], device_id={"dev": there}, device_id_type=MESH,
        )

    def asked_of(c):
        many = pl.ds(0, deck - 1 if c == planes - 1 else deck)
        return pltpu.make_async_remote_copy(
            src_ref=req.at[many], dst_ref=wanted.at[many], send_sem=ask_s.at[c],
            recv_sem=ask_r.at[decks[c]], device_id={"dev": me}, device_id_type=MESH,
        )

    for c in range(planes):
        def ask(j, carry, c=c):
            asking(c, j).start()
            return carry

        lax.fori_loop(1 if c == planes - 1 else 0, deck, ask, 0)
    wanted[me] = req[me]

    order = jnp.sum(flag(count_up((rows, 128), 1) == pos_col) * count_up((rows, 128), 0), axis=0, keepdims=True)
    order = jnp.minimum(order, float(rows - 1))
    order_v[...] = jnp.broadcast_to(order, (8, 128)).astype(jnp.int32)
    to_scalars = pltpu.make_async_copy(order_v, order_s, in_sem.at[2])
    to_scalars.start()

    small[2].wait()
    small[3].wait()
    width = size * comps
    span = size * bands
    used = width + span
    depth = tgt_depth(width, span)
    blend_row, comp_row = split_row((width, 1), 0, comps)
    blend_col, comp_col = split_row((1, width), 1, comps)
    band_row, member_row = split_row((span, 1), 0, size)
    same = flag(blend_row == blend_col)
    same_t = flag(member_row == blend_col)
    members = flag(iota((size, width), 0) == blend_col)
    unit = flag(iota((span, depth), 0) + width == iota((span, depth), 1))
    lift = flag(iota((size, depth), 1) == used)
    eye = flag(iota((width, width), 0) == iota((width, width), 1)).astype(BF16)
    gather_k = flag(iota((comps, width), 0) == comp_col).astype(BF16)
    sed_all = jnp.concatenate([sed0[b].astype(F32) for b in range(bands)], axis=1).astype(BF16)
    band_of, _ = split_row((1, bands * rows), 1, rows)
    pos_of = lanes_of(*[pos_row] * bands)
    counts = jnp.broadcast_to(count[...], (8, rows)).astype(F32).astype(BF16)

    def chosen(g):
        hit = (band_of == band_row) & (pos_of == (g * size + member_row).astype(F32))
        return flag(hit).astype(BF16)

    def every_band(column):
        return jnp.concatenate([column] * bands, axis=0)

    def sed_stepsize(total):
        flat = jnp.sum(total * total, axis=0, keepdims=True)
        return 1.0 / (jnp.sqrt(jnp.sum(members * flat, axis=1, keepdims=True)) + 1.0)

    def wide(column):
        return jnp.broadcast_to(column, (column.shape[0], 128))

    def over_groups(body, first, number, pair):
        pair = math.gcd(number, pair)

        def some(j, carry):
            stores = []
            for k in range(pair):
                stores = stores + body(first + j * pair + k)
            for ref, index, value in stores:
                ref[index] = value
            return carry

        lax.fori_loop(0, number // pair, some, 0)

    def begin(g):
        mine = pos_row == (g * size + blend_row).astype(F32)
        kept = jnp.sum(jnp.where(mine, count[...].astype(F32), 0.0), axis=1, keepdims=True)
        active = flag(comp_row.astype(F32) < kept)
        owner = flag(pos_col == (g * size + blend_col).astype(F32)).astype(BF16)
        active_t = flag(comp_col.astype(F32) < dot(counts, owner)[0:1])
        first = dot_nt(chosen(g), sed_all)
        stores = [(seds, g, dot(first.astype(BF16), gather_k) * same_t * active_t)]
        tail = flag(iota((depth - used, pixels), 0) == 0).astype(BF16)
        places = [jnp.clip(order_s[0, g * size + m], 0, rows - 1) for m in range(size)]
        for f in range(foot):
            whole = rows_of(*[morph_in[place, f].astype(F32) for place in places])
            stores.append((fit, (g, f, slice(0, width)), (whole * active).astype(BF16)))
            stores.append((fit, (g, f, slice(used, depth)), tail))
        return stores

    load_tiles.wait()
    tiles_b[...] = tiles[...].reshape(bands * tile_rows, pixels).astype(BF16)

    team = math.gcd(peers, 16)
    each = bands * held
    crowd = team * each
    stock = bands * tile_rows
    teams = [slice(k, k + team) for k in range(0, peers, team)]
    peer_col = split_row((1, crowd), 1, each)[0]
    seat_band_col, seat_rank_col = split_row((1, crowd), 1, held)
    seat_band_col = seat_band_col - peer_col * bands

    ranks = deck * each
    asker_row, seat_rank_row = split_row((ranks, 1), 0, held)
    seat_band_row = asker_row - split_row((ranks, 1), 0, each)[0] * bands

    def pick_of(h, c):
        lines = rows_of(*[jnp.broadcast_to(wanted[member(c, j)], (each, 128)) for j in range(deck)])
        seat = flag(iota((ranks, 128), 1) == h * held + seat_rank_row)
        tile = jnp.sum(lines * seat, axis=1, keepdims=True)
        at = jnp.where(tile > 0.0, tile - 1.0 + (seat_band_row * tile_rows).astype(F32), -1.0)
        return flag(count_up((ranks, stock), 1) == at).astype(BF16)

    def pick_t_of(h, who):
        lines = wanted[who].reshape(team, 128).astype(BF16)
        seat = flag(iota((128, crowd), 0) == h * held + seat_rank_col).astype(BF16)
        tile = dot(lines, seat) * flag(iota((team, crowd), 0) == peer_col)
        tile = jnp.sum(tile, axis=0, keepdims=True)
        at = jnp.where(tile > 0.0, tile - 1.0 + (seat_band_col * tile_rows).astype(F32), -1.0)
        return flag(count_up((stock, crowd), 0) == at).astype(BF16)

    fetches = [
        exchange(send.at[h], arrived.at[h], put_s.at[h], put_r.at[h]) for h in range(halves)
    ]
    for h in range(halves):
        for c in range(planes):
            if h == 0:
                asked_of(c).wait_recv()
            block = dot(pick_of(h, c), tiles_b[...]).astype(BF16)
            for j in range(deck):
                send[h, member(c, j)] = block[j * each : (j + 1) * each]
            fetches[h][0](c)
        arrived[h, me] = send[h, me]

    def morph_of(g, f):
        return fit[g, f, 0:width]

    def first_gram(g):
        total = dot_nt(morph_of(g, 0), morph_of(g, 0))
        for f in range(1, foot):
            total = total + dot_nt(morph_of(g, f), morph_of(g, f))
        total = total * same
        return [(gram, g, total.astype(BF16)), (sed_step, g, wide(sed_stepsize(total)))]

    to_scalars.wait()
    load.wait()
    over_groups(begin, 0, groups, 2)
    over_groups(first_gram, 0, groups, 4)

    crew = per_half * foot * span
    crew_row, crew_band_row = split_row((crew, 1), 0, span)
    crew_band_row, crew_member_row = split_row((crew, 1), 0, size)
    crew_band_row = crew_band_row - crew_row * bands
    crew_col, _ = split_row((1, crew), 1, span)
    crew_band_col, crew_member_col = split_row((1, crew), 1, size)
    crew_band_col = crew_band_col - crew_col * bands
    group_row = split_row((crew, 1), 0, foot * span)[0]
    group_col = split_row((1, crew), 1, foot * span)[0]
    foot_row = crew_row - group_row * foot
    foot_col = crew_col - group_col * foot
    entry_row = lanes_of(*[pos_row + f * rows for f in range(foot)])
    entry_col = rows_of(*[pos_col + f * rows for f in range(foot)])
    facts = lanes_of(
        jnp.broadcast_to(source_col, (entries, 128)), jnp.broadcast_to(rank_col, (entries, 128))
    ).astype(BF16)
    facts_t = rows_of(source_row, rank_row, jnp.zeros((6, entries), F32)).astype(BF16)

    def give_of(h, first):
        here = ((h * per_half + group_row) * size + crew_member_row + foot_row * rows).astype(F32)
        found = dot(flag(here == entry_row).astype(BF16), facts)
        at = (found[:, 0:1] - first) * each + found[:, 128:129] + (crew_band_row * held).astype(F32)
        return flag(count_up((crew, crowd), 1) == at).astype(BF16)

    def give_t_of(h, first):
        here = ((h * per_half + group_col) * size + crew_member_col + foot_col * rows).astype(F32)
        found = dot(facts_t, flag(entry_col == here).astype(BF16))
        at = (found[0:1] - first) * each + found[1:2] + (crew_band_col * held).astype(F32)
        return flag(count_up((crowd, crew), 0) == at).astype(BF16)

    def first_seds(g):
        cross = dot_nt(fit[g, 0, width:used], morph_of(g, 0))
        for f in range(1, foot):
            cross = cross + dot_nt(fit[g, f, width:used], morph_of(g, f))
        old = seds[g]
        slope = dot(old.astype(BF16), gram[g]) - cross * same_t
        sed = jnp.maximum(old - slope * every_band(sed_step[g, :, 0:1]), 0.0).astype(BF16)
        return [(seds, g, sed.astype(F32))]

    def plan_move(g):
        sed = seds[g]
        bold = sed.astype(BF16)
        small = dot_nt(bold, bold)
        flat = jnp.sum(small * small, axis=1, keepdims=True).reshape(bands, size, 1)
        step = 1.0 / (jnp.sqrt(jnp.sum(flat, axis=0)) + 1.0)
        blank = jnp.zeros((span, depth - width), F32)
        right = (unit - jnp.concatenate([sed, blank], axis=1)) * every_band(step)
        right = jnp.concatenate([right, lift * (-0.1 * step)], axis=0).astype(BF16)
        left = dot_nt(eye, jnp.concatenate([sed, members], axis=0).astype(BF16)).astype(BF16)
        return [(move, g, dot(left, right).astype(BF16))]

    def moved(g, f):
        shift = dot(move[g], fit[g, f])
        return jnp.maximum(fit[g, f, 0:width].astype(F32) + shift, 0.0).astype(BF16)

    def first_morphs(g):
        return [(fit, (g, f, slice(0, width)), moved(g, f)) for f in range(foot)]

    def second_seds(g):
        total = dot_nt(fit[g, 0, 0:used], morph_of(g, 0))
        for f in range(1, foot):
            total = total + dot_nt(fit[g, f, 0:used], morph_of(g, f))
        cross = total[width:used] * same_t
        total = total[0:width] * same
        old = seds[g]
        slope = dot(old.astype(BF16), total.astype(BF16)) - cross
        sed = jnp.maximum(old - slope * every_band(sed_stepsize(total)), 0.0).astype(BF16)
        return [(seds, g, sed.astype(F32))]

    def last_models(g):
        sed = seds[g].astype(BF16)
        return [(mod, (g, f), dot(sed, morph_of(g, f)).astype(BF16)) for f in range(foot)]

    for h in range(halves):
        for k in range(len(teams)):
            give[h, k] = give_of(h, k * team)
            give_t[h, k] = give_t_of(h, k * team)

    trips = []
    for h in range(halves):
        first = h * per_half
        fetches[h][1]()
        block = jnp.zeros((crew, pixels), F32)
        for k, who in enumerate(teams):
            come = arrived[h, who].astype(F32).reshape(crowd, pixels).astype(BF16)
            block = block + dot(give[h, k], come)
        block = block.astype(BF16).reshape(per_half, foot, span, pixels)
        fit[first : first + per_half, :, width:used] = block
        over_groups(first_seds, first, per_half, 4)
        over_groups(plan_move, first, per_half, 4)
        over_groups(first_morphs, first, per_half, 4)
        over_groups(second_seds, first, per_half, 4)
        over_groups(plan_move, first, per_half, 4)
        over_groups(first_morphs, first, per_half, 4)
        over_groups(last_models, first, per_half, 4)
        models = mod[first : first + per_half].reshape(crew, pixels)
        for k, who in enumerate(teams):
            block = dot(give_t[h, k], models)
            outb[h, who] = block.reshape(team, each, pixels).astype(BF16)
        trips.append(exchange(outb.at[h], ret.at[h], back_s.at[h], back_r.at[h]))
        for c in range(planes):
            trips[h][0](c)
        ret[h, me] = outb[h, me]

    def put_back(g, placed):
        lean = dot_nt(gather_k, seds[g].astype(BF16))
        return placed + dot(lean.astype(BF16), chosen(g))

    for h in range(halves):
        for k, who in enumerate(teams):
            pick_t[h, k] = pick_t_of(h, who)
    placed = lax.fori_loop(0, groups, put_back, jnp.zeros((comps, bands * rows), F32))
    for b in range(bands):
        sed_made[b] = placed[:, b * rows : (b + 1) * rows].astype(BF16)
    keep_sed = pltpu.make_async_copy(sed_made, sed_out, in_sem.at[0])
    keep_sed.start()

    for h in range(halves):
        trips[h][1]()
        total = jnp.zeros((stock, pixels), F32)
        for k, who in enumerate(teams):
            come = ret[h, who].astype(F32).reshape(crowd, pixels).astype(BF16)
            total = total + dot(pick_t[h, k], come)
        left = tiles if h == 0 else white
        white[...] = left[...] - total.reshape(bands, tile_rows, pixels)

    keep_white = pltpu.make_async_copy(white, white_out, in_sem.at[1])
    keep_white.start()
    squares = jnp.zeros((8, 128), F32)
    for b in range(bands):
        square = white[b] * white[b]
        for r in range(0, tile_rows, 8):
            for c in range(0, pixels, 128):
                squares = squares + square[r : r + 8, c : c + 128]

    own_row = jnp.sum(squares, axis=0, keepdims=True)
    part[...] = own_row

    place_of = me * regions + lax.axis_index("grp")

    def share(dev, grp):
        return pltpu.make_async_remote_copy(
            src_ref=part, dst_ref=parts.at[place_of], send_sem=sum_s, recv_sem=sum_r,
            device_id={"grp": grp, "dev": dev}, device_id_type=MESH,
        )

    def start_share(dev, carry):
        for grp in range(regions):
            @pl.when(dev * regions + grp != place_of)
            def _():
                share(dev, grp).start()
        return carry

    many = pl.ds(0, everyone - 1)
    shares = pltpu.make_async_remote_copy(
        src_ref=parts.at[many], dst_ref=parts.at[many], send_sem=sum_s, recv_sem=sum_r,
        device_id={"dev": me}, device_id_type=MESH,
    )
    lax.fori_loop(0, peers, start_share, 0)
    parts[place_of] = own_row
    for c in range(planes):
        asked_of(c).wait_send()
    for trip in fetches + trips:
        trip[2]()
    shares.wait_recv()
    total = jnp.sum(parts[...], axis=0)
    total = jnp.sum(jnp.sum(total, axis=1, keepdims=True), axis=0, keepdims=True)
    count_all = float(bands * tile_rows * pixels * everyone)
    scale_made[...] = jnp.broadcast_to(1.0 / jnp.sqrt(total / count_all + 1e-06), (8, 128))
    keep_scale = pltpu.make_async_copy(scale_made, scale_out, in_sem.at[2])
    keep_scale.start()
    shares.wait_send()
    keep_sed.wait()
    keep_white.wait()
    keep_scale.wait()


def finish(scale, residual, sed, white_out, sed_out):
    white_out[...] = residual[...] * scale[0:1, 0:1]
    sed_out[...] = sed[...]


def on_device(pixel_tiles, blend_source, blend_slot, component_count, sed_start, morph_start):
    peers = lax.axis_size("dev")
    regions = lax.axis_size("grp")
    rows, foot = blend_source.shape
    tile_rows, bands, pixels = pixel_tiles.shape
    comps = sed_start.shape[1]
    size = math.gcd(rows, 8)
    groups = rows // size
    halves, held = plan_slots(peers, rows, foot, bands, groups)
    width = size * comps
    span = size * bands
    depth = tgt_depth(width, span)
    vmem = pl.BlockSpec(memory_space=pltpu.VMEM)
    hbm = pl.BlockSpec(memory_space=pl.ANY)
    dma = pltpu.SemaphoreType.DMA
    team = math.gcd(peers, 16)
    crowd = team * bands * held
    crew = groups // halves * foot * span
    parcel = pltpu.VMEM((halves, peers, bands * held, pixels), BF16)
    residual, sed_final, scale = pl.pallas_call(
        functools.partial(kernel, peers, regions, halves, held, size),
        out_shape=(
            jax.ShapeDtypeStruct((bands, tile_rows, pixels), F32),
            jax.ShapeDtypeStruct((bands, comps, rows), BF16),
            jax.ShapeDtypeStruct((8, 128), F32),
        ),
        in_specs=[hbm] * 6,
        out_specs=(hbm, hbm, hbm),
        scratch_shapes=[
            pltpu.VMEM((8, 128), F32),
            pltpu.VMEM((foot, rows), jnp.int32),
            pltpu.VMEM((foot, rows), jnp.int32),
            pltpu.VMEM((1, rows), jnp.int32),
            pltpu.VMEM((bands, comps, rows), BF16),
            pltpu.VMEM((bands, tile_rows, pixels), F32),
            pltpu.VMEM((bands, comps, rows), BF16),
            pltpu.VMEM((bands, tile_rows, pixels), F32),
            pltpu.VMEM((bands * tile_rows, pixels), BF16),
            pltpu.VMEM(morph_start.shape, BF16),
            pltpu.VMEM((groups, foot, depth, pixels), BF16),
            pltpu.VMEM((groups, width, width), BF16),
            pltpu.VMEM((groups, span, width), F32),
            pltpu.VMEM((groups, size, 128), F32),
            pltpu.VMEM((groups, width, depth), BF16),
            pltpu.VMEM((groups, foot, span, pixels), BF16),
            pltpu.VMEM((halves, peers // team, crew, crowd), BF16),
            pltpu.VMEM((halves, peers // team, crowd, crew), BF16),
            pltpu.VMEM((halves, peers // team, bands * tile_rows, crowd), BF16),
            pltpu.VMEM((8, 128), jnp.int32),
            pltpu.SMEM((8, 128), jnp.int32),
            pltpu.VMEM((peers, 1, 128), F32),
            pltpu.VMEM((peers, 1, 128), F32),
            parcel,
            parcel,
            parcel,
            parcel,
            pltpu.VMEM((1, 128), F32),
            pltpu.VMEM((peers * regions, 1, 128), F32),
            dma((7,)),
            dma((4,)),
            dma((4,)),
            dma((halves,)),
            dma((halves,)),
            dma((halves,)),
            dma((halves,)),
            dma,
            dma,
        ],
        compiler_params=pltpu.CompilerParams(
            collective_id=0, has_side_effects=True, vmem_limit_bytes=40 * 1024 * 1024
        ),
    )(
        *[
            pltpu.with_memory_space_constraint(given, pltpu.HBM)
            for given in (
                jnp.transpose(pixel_tiles, (1, 0, 2)),
                jnp.transpose(blend_source),
                jnp.transpose(blend_slot),
                component_count.reshape(1, rows),
                jnp.transpose(sed_start, (2, 1, 0)),
                morph_start,
            )
        ]
    )
    white, sed_final = pl.pallas_call(
        finish,
        out_shape=(
            jax.ShapeDtypeStruct((bands, tile_rows, pixels), F32),
            jax.ShapeDtypeStruct((bands, comps, rows), BF16),
        ),
        in_specs=[vmem, vmem, vmem],
        out_specs=(vmem, vmem),
        compiler_params=pltpu.CompilerParams(vmem_limit_bytes=8 * 1024 * 1024),
    )(scale, residual, sed_final)
    return jnp.transpose(white, (1, 0, 2)), jnp.transpose(sed_final, (2, 1, 0))


def solution(mesh):
    placed = (
        P(("grp", "dev"), None, None),
        P(("grp", "dev"), None),
        P(("grp", "dev"), None),
        P(("grp", "dev")),
        P(("grp", "dev"), None, None),
        P(("grp", "dev"), None, None, None),
    )
    return jax.shard_map(
        on_device,
        mesh=mesh,
        in_specs=placed,
        out_specs=(P(("grp", "dev"), None, None), P(("grp", "dev"), None, None)),
        check_vma=False,
    )
```

```python
import functools
import math

import jax
import jax.numpy as jnp
from jax import lax
from jax.experimental import pallas as pl
from jax.experimental.pallas import tpu as pltpu
from jax.sharding import PartitionSpec as P

F32 = jnp.float32
BF16 = jnp.bfloat16
MESH = pl.DeviceIdType.MESH


def dot(a, b):
    return jnp.dot(a, b, preferred_element_type=F32)


def dot_nt(a, b):
    return lax.dot_general(a, b, (((1,), (1,)), ((), ())), preferred_element_type=F32)


def iota(shape, dimension):
    return lax.broadcasted_iota(jnp.int32, shape, dimension)


def count_up(shape, dimension):
    return iota(shape, dimension).astype(F32)


def split_row(shape, dimension, width):
    place = iota(shape, dimension)
    out = jnp.zeros(shape, jnp.int32)
    for cut in range(width, shape[dimension], width):
        out = out + (place >= cut).astype(jnp.int32)
    return out, place - out * width


def flag(condition):
    return condition.astype(F32)


def lanes_of(*parts):
    return parts[0] if len(parts) == 1 else jnp.concatenate(parts, axis=1)


def rows_of(*parts):
    return parts[0] if len(parts) == 1 else jnp.concatenate(parts, axis=0)


def tgt_depth(width, span):
    return (width + span) // 16 * 16 + 16


CUTS = 2


def plan_slots(peers, rows, foot, bands, groups):
    entries = rows * foot
    capacity = max(2, (entries + peers - 1) // peers)
    even = foot == 2 and peers * capacity == entries and capacity % 4 == 0
    halves = 2 if even and groups % 2 == 0 and entries == 128 else 1
    held = capacity // halves
    while held * bands % 8:
        held = held + 1
    return halves, held


def turn(*lines):
    n = lines[0].shape[1]
    return jnp.transpose(rows_of(*lines, jnp.zeros((8 - len(lines), n), F32)))


def partners(col, row):
    shape = (col.shape[0], row.shape[1])
    here, there = iota(shape, 0), iota(shape, 1)
    alike = flag(col == row)
    rank_col = jnp.sum(alike * flag(there < here), axis=1, keepdims=True)
    rank_row = jnp.sum(alike * flag(there > here), axis=0, keepdims=True)
    level = flag(jnp.floor(rank_col * 0.5) == jnp.floor(rank_row * 0.5))
    pair = alike * level * flag(here != there)
    found = jnp.sum(pair * here.astype(F32), axis=0, keepdims=True)
    return jnp.broadcast_to(found, (8, shape[1])).astype(jnp.int32)


def follow(values, at):
    return jnp.take_along_axis(values, at, axis=1)


def lowest(step, length):
    least = iota(step.shape, 1)
    reach = 1
    while reach < length:
        least = jnp.minimum(least, follow(least, step))
        step = follow(step, step)
        reach = reach * 2
    return least


def halve(source_col, source_row, n):
    def swap(values):
        return jnp.concatenate([values[:, n:], values[:, :n]], axis=1)

    least = lowest(swap(partners(source_col, source_row)), n)
    tail = (least < swap(least))[0:1]
    other_row = swap(source_row)
    tail_row = jnp.where(tail, source_row, other_row)
    head_row = jnp.where(tail, other_row, source_row)
    turned = turn(tail_row, head_row)[:n]
    lane = iota((n, 2 * n), 1)
    tails = partners(turned[:, 0:1], jnp.where(lane[0:1] < n, tail_row, -1.0))
    heads = partners(turned[:, 1:2], jnp.where(lane[0:1] < n, head_row, -1.0))
    least = lowest(follow(heads, tails), n // 2)
    return flag(least >= follow(least, tails))[0:1]


def kernel(
    peers, regions, halves, held, size,
    tiles_hbm, source_hbm, slot_hbm, count_hbm, sed_hbm, morph_hbm, white_out, sed_out, scale_out, scale_made, source, slot, count, sed0,
    white, sed_made, tiles, tiles_b, morph_in, fit, gram, seds, sed_step, move, mod, give, give_t, pick_t, order_v, order_s, req, wanted, send, arrived, outb, ret, part, parts,
    in_sem, ask_s, ask_r, put_s, put_r, back_s, back_r, sum_s, sum_r,
):
    bands, tile_rows, pixels = tiles.shape
    foot, rows = source.shape
    comps = sed0.shape[1]
    groups = rows // size
    per_half = groups // halves
    me = lax.axis_index("dev")
    everyone = peers * regions
    small = [
        pltpu.make_async_copy(given, kept, in_sem.at[3 + i])
        for i, (given, kept) in enumerate(
            ((source_hbm, source), (slot_hbm, slot), (count_hbm, count), (sed_hbm, sed0))
        )
    ]
    for copy in small:
        copy.start()
    load_tiles = pltpu.make_async_copy(tiles_hbm, tiles, in_sem.at[0])
    load_tiles.start()
    load = pltpu.make_async_copy(morph_hbm, morph_in, in_sem.at[1])
    load.start()
    barrier = pltpu.get_barrier_semaphore()

    place_of = me * regions + lax.axis_index("grp")

    def greet(dev, carry):
        for grp in range(regions):
            @pl.when(dev * regions + grp != place_of)
            def _():
                pl.semaphore_signal(
                    barrier, inc=1, device_id={"grp": grp, "dev": dev}, device_id_type=MESH
                )
        return carry

    lax.fori_loop(0, peers, greet, 0)

    small[0].wait()
    small[1].wait()
    entries = foot * rows
    source_row = lanes_of(*[source[f : f + 1, :] for f in range(foot)]).astype(F32)
    slot_row = lanes_of(*[slot[f : f + 1, :] for f in range(foot)]).astype(F32)
    turned = turn(source_row, slot_row)
    source_col = turned[:, 0:1]
    slot_col = turned[:, 1:2]
    before = flag(iota((entries, entries), 1) < iota((entries, entries), 0))
    after = flag(iota((entries, entries), 1) > iota((entries, entries), 0))
    alike = flag(source_col == source_row)
    if halves == 2:
        half = halve(source_col, source_row, rows)
        half_col = turn(half)[:rows, 0:1]
        half_row = half[:, :rows]
        alone = flag(half_col == half_row)
        base = rows // 2
        pos_col = half_col * base + jnp.sum(alone * before[:rows, :rows], axis=1, keepdims=True)
        pos_row = half_row * base + jnp.sum(alone * after[:rows, :rows], axis=0, keepdims=True)
        both_col = rows_of(half_col, half_col)
        both_row = lanes_of(half_row, half_row)
        alike = alike * flag(both_col == both_row)
        rank_col = jnp.sum(alike * before, axis=1, keepdims=True)
        rank_row = jnp.sum(alike * after, axis=0, keepdims=True)
        lane_col = both_col * held + rank_col
    else:
        pos_col = count_up((rows, 1), 0)
        pos_row = count_up((1, rows), 1)
        rank_col = jnp.sum(alike * before, axis=1, keepdims=True)
        rank_row = jnp.sum(alike * after, axis=0, keepdims=True)
        lane_col = rank_col
    named = flag(count_up((peers, entries), 0) == source_row)
    asked = flag(count_up((entries, 128), 1) == lane_col) * (slot_col + 1.0)
    req[...] = dot(named.astype(BF16), asked.astype(BF16)).reshape(peers, 1, 128)
    pl.semaphore_wait(barrier, everyone - 1)

    planes = 4 if peers % 4 == 0 else 1
    deck = peers // planes
    level = lax.div(me, deck)
    spot = lax.rem(me, deck)
    upper = lax.div(level, 2)
    if planes == 4:
        decks = [2 - upper, 3 - 3 * upper, 4 * upper + 1 - level, level]
    else:
        decks = [level]

    def member(c, j):
        return decks[c] * deck + lax.rem(spot + j, deck)

    def exchange(src, dst, send_sem, recv_sem):
        def copy(from_here, to_there, there=me):
            return pltpu.make_async_remote_copy(
                src_ref=src.at[from_here], dst_ref=dst.at[to_there], send_sem=send_sem,
                recv_sem=recv_sem, device_id={"dev": there}, device_id_type=MESH,
            )

        def start(c, low=0, high=deck):
            def body(j, carry):
                there = member(c, j)
                copy(there, me, there).start()
                return carry

            lax.fori_loop(max(low, 1 if c == planes - 1 else 0), high, body, 0)

        others = pl.ds(0, peers - 1)
        return start, copy(others, others).wait_recv, copy(others, others).wait_send

    def asking(c, j, facing):
        there = member(c, j)
        return pltpu.make_async_remote_copy(
            src_ref=req.at[there], dst_ref=wanted.at[me], send_sem=ask_s.at[c, facing],
            recv_sem=ask_r.at[level, facing], device_id={"dev": there}, device_id_type=MESH,
        )

    def asked_of(c, facing):
        many = pl.ds(0, 1 if facing else deck - 1)
        return pltpu.make_async_remote_copy(
            src_ref=req.at[many], dst_ref=wanted.at[many], send_sem=ask_s.at[c, facing],
            recv_sem=ask_r.at[decks[c], facing], device_id={"dev": me}, device_id_type=MESH,
        )

    for c in range(planes):
        def ask(j, carry, c=c):
            asking(c, j, 0).start()
            return carry

        if c < planes - 1:
            asking(c, 0, 1).start()
        lax.fori_loop(1, deck, ask, 0)
    wanted[me] = req[me]

    order = jnp.sum(flag(count_up((rows, 128), 1) == pos_col) * count_up((rows, 128), 0), axis=0, keepdims=True)
    order = jnp.minimum(order, float(rows - 1))
    order_v[...] = jnp.broadcast_to(order, (8, 128)).astype(jnp.int32)
    to_scalars = pltpu.make_async_copy(order_v, order_s, in_sem.at[2])
    to_scalars.start()

    small[2].wait()
    small[3].wait()
    width = size * comps
    span = size * bands
    used = width + span
    depth = tgt_depth(width, span)
    blend_row, comp_row = split_row((width, 1), 0, comps)
    blend_col, comp_col = split_row((1, width), 1, comps)
    band_row, member_row = split_row((span, 1), 0, size)
    same = flag(blend_row == blend_col)
    same_t = flag(member_row == blend_col)
    members = flag(iota((size, width), 0) == blend_col)
    unit = flag(iota((span, depth), 0) + width == iota((span, depth), 1))
    lift = flag(iota((size, depth), 1) == used)
    eye = flag(iota((width, width), 0) == iota((width, width), 1)).astype(BF16)
    gather_k = flag(iota((comps, width), 0) == comp_col).astype(BF16)
    sed_all = jnp.concatenate([sed0[b].astype(F32) for b in range(bands)], axis=1).astype(BF16)
    band_of, _ = split_row((1, bands * rows), 1, rows)
    pos_of = lanes_of(*[pos_row] * bands)
    counts = jnp.broadcast_to(count[...], (8, rows)).astype(F32).astype(BF16)

    def chosen(g):
        hit = (band_of == band_row) & (pos_of == (g * size + member_row).astype(F32))
        return flag(hit).astype(BF16)

    def every_band(column):
        return jnp.concatenate([column] * bands, axis=0)

    def sed_stepsize(total):
        flat = jnp.sum(total * total, axis=0, keepdims=True)
        return 1.0 / (jnp.sqrt(jnp.sum(members * flat, axis=1, keepdims=True)) + 1.0)

    def wide(column):
        return jnp.broadcast_to(column, (column.shape[0], 128))

    def over_groups(body, first, number, pair):
        pair = math.gcd(number, pair)

        def some(j, carry):
            stores = []
            for k in range(pair):
                stores = stores + body(first + j * pair + k)
            for ref, index, value in stores:
                ref[index] = value
            return carry

        lax.fori_loop(0, number // pair, some, 0)

    def begin(g):
        mine = pos_row == (g * size + blend_row).astype(F32)
        kept = jnp.sum(jnp.where(mine, count[...].astype(F32), 0.0), axis=1, keepdims=True)
        active = flag(comp_row.astype(F32) < kept)
        owner = flag(pos_col == (g * size + blend_col).astype(F32)).astype(BF16)
        active_t = flag(comp_col.astype(F32) < dot(counts, owner)[0:1])
        first = dot_nt(chosen(g), sed_all)
        stores = [(seds, g, dot(first.astype(BF16), gather_k) * same_t * active_t)]
        tail = flag(iota((depth - used, pixels), 0) == 0).astype(BF16)
        places = [jnp.clip(order_s[0, g * size + m], 0, rows - 1) for m in range(size)]
        for f in range(foot):
            whole = rows_of(*[morph_in[place, f].astype(F32) for place in places])
            stores.append((fit, (g, f, slice(0, width)), (whole * active).astype(BF16)))
            stores.append((fit, (g, f, slice(used, depth)), tail))
        return stores

    load_tiles.wait()
    tiles_b[...] = tiles[...].reshape(bands * tile_rows, pixels).astype(BF16)

    team = math.gcd(peers, 16)
    each = bands * held
    crowd = team * each
    stock = bands * tile_rows
    teams = [slice(k, k + team) for k in range(0, peers, team)]
    peer_col = split_row((1, crowd), 1, each)[0]
    seat_band_col, seat_rank_col = split_row((1, crowd), 1, held)
    seat_band_col = seat_band_col - peer_col * bands

    ranks = deck * each
    asker_row, seat_rank_row = split_row((ranks, 1), 0, held)
    seat_band_row = asker_row - split_row((ranks, 1), 0, each)[0] * bands

    def pick_of(h, c, who):
        lines = rows_of(*[jnp.broadcast_to(wanted[member(c, j)], (each, 128)) for j in who])
        n = len(who) * each
        seat = flag(iota((n, 128), 1) == h * held + seat_rank_row[:n])
        tile = jnp.sum(lines * seat, axis=1, keepdims=True)
        at = jnp.where(tile > 0.0, tile - 1.0 + (seat_band_row[:n] * tile_rows).astype(F32), -1.0)
        return flag(count_up((n, stock), 1) == at).astype(BF16)

    def pick_t_of(h, who):
        lines = wanted[who].reshape(team, 128).astype(BF16)
        seat = flag(iota((128, crowd), 0) == h * held + seat_rank_col).astype(BF16)
        tile = dot(lines, seat) * flag(iota((team, crowd), 0) == peer_col)
        tile = jnp.sum(tile, axis=0, keepdims=True)
        at = jnp.where(tile > 0.0, tile - 1.0 + (seat_band_col * tile_rows).astype(F32), -1.0)
        return flag(count_up((stock, crowd), 0) == at).astype(BF16)

    fetches = [
        exchange(send.at[h], arrived.at[h], put_s.at[h], put_r.at[h]) for h in range(halves)
    ]
    for h in range(halves):
        pieces = [(c, 0, deck) for c in range(planes)]
        if h == 0 and planes > 1:
            pieces = [(0, 0, 1), (1, 0, 1), (0, 1, deck), (1, 1, deck)] + pieces[2:]
        for c, low, high in pieces:
            if h == 0 and low == 0 and c < planes - 1:
                asked_of(c, 1).wait_recv()
            if h == 0 and high > 1:
                asked_of(c, 0).wait_recv()
            who = range(low, high)
            block = dot(pick_of(h, c, who), tiles_b[...]).astype(BF16)
            for i, j in enumerate(who):
                send[h, member(c, j)] = block[i * each : (i + 1) * each]
            fetches[h][0](c, low, high)
        arrived[h, me] = send[h, me]

    def morph_of(g, f):
        return fit[g, f, 0:width]

    def first_gram(g):
        total = dot_nt(morph_of(g, 0), morph_of(g, 0))
        for f in range(1, foot):
            total = total + dot_nt(morph_of(g, f), morph_of(g, f))
        total = total * same
        return [(gram, g, total.astype(BF16)), (sed_step, g, wide(sed_stepsize(total)))]

    to_scalars.wait()
    load.wait()
    over_groups(begin, 0, groups, 2)
    over_groups(first_gram, 0, groups, 4)

    crew = per_half * foot * span
    crew_row, crew_band_row = split_row((crew, 1), 0, span)
    crew_band_row, crew_member_row = split_row((crew, 1), 0, size)
    crew_band_row = crew_band_row - crew_row * bands
    crew_col, _ = split_row((1, crew), 1, span)
    crew_band_col, crew_member_col = split_row((1, crew), 1, size)
    crew_band_col = crew_band_col - crew_col * bands
    group_row = split_row((crew, 1), 0, foot * span)[0]
    group_col = split_row((1, crew), 1, foot * span)[0]
    foot_row = crew_row - group_row * foot
    foot_col = crew_col - group_col * foot
    entry_row = lanes_of(*[pos_row + f * rows for f in range(foot)])
    entry_col = rows_of(*[pos_col + f * rows for f in range(foot)])
    facts = lanes_of(
        jnp.broadcast_to(source_col, (entries, 128)), jnp.broadcast_to(rank_col, (entries, 128))
    ).astype(BF16)
    facts_t = rows_of(source_row, rank_row, jnp.zeros((6, entries), F32)).astype(BF16)

    def give_of(h, first):
        here = ((h * per_half + group_row) * size + crew_member_row + foot_row * rows).astype(F32)
        found = dot(flag(here == entry_row).astype(BF16), facts)
        at = (found[:, 0:1] - first) * each + found[:, 128:129] + (crew_band_row * held).astype(F32)
        return flag(count_up((crew, crowd), 1) == at).astype(BF16)

    def give_t_of(h, first):
        here = ((h * per_half + group_col) * size + crew_member_col + foot_col * rows).astype(F32)
        found = dot(facts_t, flag(entry_col == here).astype(BF16))
        at = (found[0:1] - first) * each + found[1:2] + (crew_band_col * held).astype(F32)
        return flag(count_up((crowd, crew), 0) == at).astype(BF16)

    def first_seds(g):
        cross = dot_nt(fit[g, 0, width:used], morph_of(g, 0))
        for f in range(1, foot):
            cross = cross + dot_nt(fit[g, f, width:used], morph_of(g, f))
        old = seds[g]
        slope = dot(old.astype(BF16), gram[g]) - cross * same_t
        sed = jnp.maximum(old - slope * every_band(sed_step[g, :, 0:1]), 0.0).astype(BF16)
        return [(seds, g, sed.astype(F32))]

    def plan_move(g):
        sed = seds[g]
        bold = sed.astype(BF16)
        small = dot_nt(bold, bold)
        flat = jnp.sum(small * small, axis=1, keepdims=True).reshape(bands, size, 1)
        step = 1.0 / (jnp.sqrt(jnp.sum(flat, axis=0)) + 1.0)
        blank = jnp.zeros((span, depth - width), F32)
        right = (unit - jnp.concatenate([sed, blank], axis=1)) * every_band(step)
        right = jnp.concatenate([right, lift * (-0.1 * step)], axis=0).astype(BF16)
        left = dot_nt(eye, jnp.concatenate([sed, members], axis=0).astype(BF16)).astype(BF16)
        return [(move, g, dot(left, right).astype(BF16))]

    def next_morphs(lanes):
        def body(g):
            stores = []
            for f in range(foot):
                shift = dot(move[g], fit[g, f, :, lanes])
                new = jnp.maximum(fit[g, f, 0:width, lanes].astype(F32) + shift, 0.0)
                stores.append((fit, (g, f, slice(0, width), lanes), new.astype(BF16)))
            return stores

        return body

    def second_seds(g):
        total = dot_nt(fit[g, 0, 0:used], morph_of(g, 0))
        for f in range(1, foot):
            total = total + dot_nt(fit[g, f, 0:used], morph_of(g, f))
        cross = total[width:used] * same_t
        total = total[0:width] * same
        old = seds[g]
        slope = dot(old.astype(BF16), total.astype(BF16)) - cross
        sed = jnp.maximum(old - slope * every_band(sed_stepsize(total)), 0.0).astype(BF16)
        return [(seds, g, sed.astype(F32))]

    def last_models(lanes):
        def body(g):
            sed = seds[g].astype(BF16)
            return [
                (mod, (g, f, slice(None), lanes), dot(sed, fit[g, f, 0:width, lanes]).astype(BF16))
                for f in range(foot)
            ]

        return body

    everything = slice(0, pixels)
    window = pixels // CUTS
    cuts = [slice(c * window, (c + 1) * window) for c in range(CUTS)]

    for h in range(halves):
        for k in range(len(teams)):
            give[h, k] = give_of(h, k * team)
            give_t[h, k] = give_t_of(h, k * team)

    trips = []
    for h in range(halves):
        first = h * per_half
        fetches[h][1]()
        block = jnp.zeros((crew, pixels), F32)
        for k, who in enumerate(teams):
            come = arrived[h, who].astype(F32).reshape(crowd, pixels).astype(BF16)
            block = block + dot(give[h, k], come)
        block = block.astype(BF16).reshape(per_half, foot, span, pixels)
        fit[first : first + per_half, :, width:used] = block
        over_groups(first_seds, first, per_half, 4)
        over_groups(plan_move, first, per_half, 4)
        over_groups(next_morphs(everything), first, per_half, 4)
        over_groups(second_seds, first, per_half, 4)
        over_groups(plan_move, first, per_half, 4)
        for i, lanes in enumerate(cuts):
            over_groups(next_morphs(lanes), first, per_half, 4)
            over_groups(last_models(lanes), first, per_half, 4)
            models = mod[first : first + per_half, :, :, lanes].reshape(crew, window)
            for k, who in enumerate(teams):
                block = dot(give_t[h, k], models)
                outb[h, i, who] = block.reshape(team, each, window).astype(BF16)
            trips.append(exchange(outb.at[h, i], ret.at[h, i], back_s.at[h, i], back_r.at[h, i]))
            for c in range(planes):
                trips[-1][0](c)
            ret[h, i, me] = outb[h, i, me]

    def put_back(g, placed):
        lean = dot_nt(gather_k, seds[g].astype(BF16))
        return placed + dot(lean.astype(BF16), chosen(g))

    for h in range(halves):
        for k, who in enumerate(teams):
            pick_t[h, k] = pick_t_of(h, who)
    placed = lax.fori_loop(0, groups, put_back, jnp.zeros((comps, bands * rows), F32))
    for b in range(bands):
        sed_made[b] = placed[:, b * rows : (b + 1) * rows].astype(BF16)
    keep_sed = pltpu.make_async_copy(sed_made, sed_out, in_sem.at[0])
    keep_sed.start()

    squares = jnp.zeros((8, 128), F32)
    for h in range(halves):
        for i, lanes in enumerate(cuts):
            trips[h * CUTS + i][1]()
            total = jnp.zeros((stock, window), F32)
            for k, who in enumerate(teams):
                come = ret[h, i, who].astype(F32).reshape(crowd, window).astype(BF16)
                total = total + dot(pick_t[h, k], come)
            total = total.reshape(bands, tile_rows, window)
            left = tiles if h == 0 else white
            for b in range(bands):
                rest = left[b, :, lanes] - total[b]
                white[b, :, lanes] = rest
                if h == halves - 1:
                    square = rest * rest
                    for r in range(0, tile_rows, 8):
                        for c in range(0, window, 128):
                            squares = squares + square[r : r + 8, c : c + 128]

    keep_white = pltpu.make_async_copy(white, white_out, in_sem.at[1])
    keep_white.start()
    own_row = jnp.sum(squares, axis=0, keepdims=True)
    part[...] = own_row

    def share(dev, grp):
        return pltpu.make_async_remote_copy(
            src_ref=part, dst_ref=parts.at[place_of], send_sem=sum_s, recv_sem=sum_r,
            device_id={"grp": grp, "dev": dev}, device_id_type=MESH,
        )

    def start_share(dev, carry):
        for grp in range(regions):
            @pl.when(dev * regions + grp != place_of)
            def _():
                share(dev, grp).start()
        return carry

    many = pl.ds(0, everyone - 1)
    shares = pltpu.make_async_remote_copy(
        src_ref=parts.at[many], dst_ref=parts.at[many], send_sem=sum_s, recv_sem=sum_r,
        device_id={"dev": me}, device_id_type=MESH,
    )
    lax.fori_loop(0, peers, start_share, 0)
    parts[place_of] = own_row
    for c in range(planes):
        asked_of(c, 0).wait_send()
        if c < planes - 1:
            asked_of(c, 1).wait_send()
    for trip in fetches + trips:
        trip[2]()
    shares.wait_recv()
    total = jnp.sum(parts[...], axis=0)
    total = jnp.sum(jnp.sum(total, axis=1, keepdims=True), axis=0, keepdims=True)
    count_all = float(bands * tile_rows * pixels * everyone)
    scale_made[...] = jnp.broadcast_to(1.0 / jnp.sqrt(total / count_all + 1e-06), (8, 128))
    keep_scale = pltpu.make_async_copy(scale_made, scale_out, in_sem.at[2])
    keep_scale.start()
    shares.wait_send()
    keep_sed.wait()
    keep_white.wait()
    keep_scale.wait()


def finish(scale, residual, sed, white_out, sed_out):
    white_out[...] = residual[...] * scale[0:1, 0:1]
    sed_out[...] = sed[...]


def on_device(pixel_tiles, blend_source, blend_slot, component_count, sed_start, morph_start):
    peers = lax.axis_size("dev")
    regions = lax.axis_size("grp")
    rows, foot = blend_source.shape
    tile_rows, bands, pixels = pixel_tiles.shape
    comps = sed_start.shape[1]
    size = math.gcd(rows, 8)
    groups = rows // size
    halves, held = plan_slots(peers, rows, foot, bands, groups)
    width = size * comps
    span = size * bands
    depth = tgt_depth(width, span)
    vmem = pl.BlockSpec(memory_space=pltpu.VMEM)
    hbm = pl.BlockSpec(memory_space=pl.ANY)
    dma = pltpu.SemaphoreType.DMA
    team = math.gcd(peers, 16)
    crowd = team * bands * held
    crew = groups // halves * foot * span
    parcel = pltpu.VMEM((halves, peers, bands * held, pixels), BF16)
    returned = pltpu.VMEM((halves, CUTS, peers, bands * held, pixels // CUTS), BF16)
    residual, sed_final, scale = pl.pallas_call(
        functools.partial(kernel, peers, regions, halves, held, size),
        out_shape=(
            jax.ShapeDtypeStruct((bands, tile_rows, pixels), F32),
            jax.ShapeDtypeStruct((bands, comps, rows), BF16),
            jax.ShapeDtypeStruct((8, 128), F32),
        ),
        in_specs=[hbm] * 6,
        out_specs=(hbm, hbm, hbm),
        scratch_shapes=[
            pltpu.VMEM((8, 128), F32),
            pltpu.VMEM((foot, rows), jnp.int32),
            pltpu.VMEM((foot, rows), jnp.int32),
            pltpu.VMEM((1, rows), jnp.int32),
            pltpu.VMEM((bands, comps, rows), BF16),
            pltpu.VMEM((bands, tile_rows, pixels), F32),
            pltpu.VMEM((bands, comps, rows), BF16),
            pltpu.VMEM((bands, tile_rows, pixels), F32),
            pltpu.VMEM((bands * tile_rows, pixels), BF16),
            pltpu.VMEM(morph_start.shape, BF16),
            pltpu.VMEM((groups, foot, depth, pixels), BF16),
            pltpu.VMEM((groups, width, width), BF16),
            pltpu.VMEM((groups, span, width), F32),
            pltpu.VMEM((groups, size, 128), F32),
            pltpu.VMEM((groups, width, depth), BF16),
            pltpu.VMEM((groups, foot, span, pixels), BF16),
            pltpu.VMEM((halves, peers // team, crew, crowd), BF16),
            pltpu.VMEM((halves, peers // team, crowd, crew), BF16),
            pltpu.VMEM((halves, peers // team, bands * tile_rows, crowd), BF16),
            pltpu.VMEM((8, 128), jnp.int32),
            pltpu.SMEM((8, 128), jnp.int32),
            pltpu.VMEM((peers, 1, 128), F32),
            pltpu.VMEM((peers, 1, 128), F32),
            parcel,
            parcel,
            returned,
            returned,
            pltpu.VMEM((1, 128), F32),
            pltpu.VMEM((peers * regions, 1, 128), F32),
            dma((7,)),
            dma((4, 2)),
            dma((4, 2)),
            dma((halves,)),
            dma((halves,)),
            dma((halves, CUTS)),
            dma((halves, CUTS)),
            dma,
            dma,
        ],
        compiler_params=pltpu.CompilerParams(
            collective_id=0, has_side_effects=True, vmem_limit_bytes=40 * 1024 * 1024
        ),
    )(
        *[
            pltpu.with_memory_space_constraint(given, pltpu.HBM)
            for given in (
                jnp.transpose(pixel_tiles, (1, 0, 2)),
                jnp.transpose(blend_source),
                jnp.transpose(blend_slot),
                component_count.reshape(1, rows),
                jnp.transpose(sed_start, (2, 1, 0)),
                morph_start,
            )
        ]
    )
    white, sed_final = pl.pallas_call(
        finish,
        out_shape=(
            jax.ShapeDtypeStruct((bands, tile_rows, pixels), F32),
            jax.ShapeDtypeStruct((bands, comps, rows), BF16),
        ),
        in_specs=[vmem, vmem, vmem],
        out_specs=(vmem, vmem),
        compiler_params=pltpu.CompilerParams(vmem_limit_bytes=8 * 1024 * 1024),
    )(scale, residual, sed_final)
    return jnp.transpose(white, (1, 0, 2)), jnp.transpose(sed_final, (2, 1, 0))


def solution(mesh):
    placed = (
        P(("grp", "dev"), None, None),
        P(("grp", "dev"), None),
        P(("grp", "dev"), None),
        P(("grp", "dev")),
        P(("grp", "dev"), None, None),
        P(("grp", "dev"), None, None, None),
    )
    return jax.shard_map(
        on_device,
        mesh=mesh,
        in_specs=placed,
        out_specs=(P(("grp", "dev"), None, None), P(("grp", "dev"), None, None)),
        check_vma=False,
    )
```
